768 devices in a mesh: dp: 24 (over z, x_hi), expert: 32 (over y, x_lo, core).
Axes of the slice: x: 4 (x_hi: 2, x_lo: 2; x = x_hi * 2 + x_lo), y: 8, z: 12, core: 2. Of those that a mesh axis runs over, the one named last changes fastest.
Arguments:
- grad_output: bfloat16 [32, 48, 3840], P('expert', None, 'dp'), may hold values from -6 to 6
- router_logits: float32 [32, 48, 128], P('expert'), may hold values from -8 to 8
- expert_ids: int32 [32, 48, 8], P('expert'), may hold values from 0 to 127, all different within a row; in each aligned block of 48 rows (0 to 47, 48 to 95, ..., all dimensions but the last counted through in order) at most 6 rows name the same one
- router_input: bfloat16 [32, 48, 3840], P('expert', 'dp'), may hold values from -6 to 6
- router_weight: bfloat16 [128, 3840], P(None, 'dp'), may hold values from -0.09375 to 0.09375
- gate_weight: bfloat16 [128, 3840, 1024], P('expert', 'dp'), may hold values from -0.09375 to 0.09375
- up_weight: bfloat16 [128, 3840, 1024], P('expert', 'dp'), may hold values from -0.09375 to 0.09375
- down_weight: bfloat16 [128, 1024, 3840], P('expert', None, 'dp'), may hold values from -0.1875 to 0.1875
- gate_saved: bfloat16 [128, 192, 1024], P('expert'), may hold values from -6 to 6
- up_saved: bfloat16 [128, 192, 1024], P('expert'), may hold values from -6 to 6
Outputs:
- grad_input: bfloat16 [32, 48, 3840], P('expert', None, 'dp')
- grad_router: float32 [128, 3840], P('expert', 'dp')
The draws below stay inside these ranges and needn't reach their ends.
Inputs may be any that keep to these rules, and one draw needn't show every extreme that they name: `expert_ids`: within one token group (the 48 tokens of one index of expert, in order), no expert is named more than 6 times, a bound that some block reaches; every row names 8 different experts.
All inputs are finite; a program needn't handle non-finite values.
Results may differ from the reference program's by a relative error of at most 0.008.
Values may be sent and summed in bfloat16 or wider, within the bound.
A program may use at most 32 MiB of HBM per device.

```python
import math
import jax
import jax.numpy as jnp
import numpy as np
from jax import lax

D = 3840
F = 1024
TOP = 8
EXPERTS = 128
GROUP = 48
MOST = 6
SLOTS = 192
N_EXPERT = 32


def level_of(own_key, extent, pieces, smallest, top_value):
    def one(axis_at, parts):
        steps = jax.random.uniform(jax.random.fold_in(jax.random.fold_in(own_key, 6), axis_at), (parts,), jnp.float32, smallest / len(pieces), top_value / len(pieces))
        return jnp.repeat(jnp.exp(steps), extent[axis_at] // parts).reshape((-1,) + (1,) * (len(extent) - axis_at - 1))

    loudness = one(*pieces[0])
    for cut in pieces[1:]:
        loudness = loudness * one(*cut)
    return loudness


def routed_block(stream_key, own, number, rows, count, top, limit, lean):
    order = jax.random.permutation(stream_key, count)
    packed, usual = portions_of(count, rows * top, limit, lean, True), portions_of(count, rows * top, limit, lean, False)
    places = jnp.arange(count)

    def named(tallies, offset_by):
        used = int((tallies > 0).sum())
        fixed = max(1, used // 4)
        shifted = fixed + (places - fixed + offset_by * (used - fixed)) % max(1, count - fixed)
        return jnp.zeros((count,), jnp.int32).at[order[jnp.where(places < fixed, places, shifted)]].set(jnp.asarray(tallies, jnp.int32))

    tallies = jnp.where(number % 4 == 0, named(packed, number // 4), named(usual, number - number // 4 - 1))
    mixed = jax.random.permutation(jax.random.fold_in(own, 3), count)
    donor, sink = mixed[0:count // 2 * 2:2], mixed[1:count // 2 * 2:2]
    slack = jnp.minimum(tallies[donor] - 1, limit - tallies[sink]) // 2
    slack = jnp.where((donor == order[0]) | (sink == order[0]) | (tallies[sink] == 0), 0, jnp.maximum(slack, 0))
    shifted = jax.random.randint(jax.random.fold_in(own, 4), (count // 2,), 0, 1 << 20) % (slack + 1)
    tallies = tallies.at[donor].add(-shifted).at[sink].add(shifted)
    labels = jnp.searchsorted(jnp.cumsum(tallies), jnp.arange(rows * top), side="right").astype(jnp.int32)
    grid = labels.reshape(top, rows).T
    grid = grid[jax.random.permutation(jax.random.fold_in(own, 1), rows)]
    offset_by = jax.random.randint(jax.random.fold_in(own, 2), (rows, 1), 0, top)
    return jnp.take_along_axis(grid, (jnp.arange(top)[None, :] + offset_by) % top, axis=1)


def portions_of(number_of, total, reach, skew, full):
    weights = [(1 << 20) // math.isqrt(rank ** skew) + 1 for rank in range(1, number_of + 1)]
    largest = reach if full else min(reach, max(-(-total // number_of), total * weights[0] // sum(weights)))
    least = 1 if total - largest >= number_of - 1 else 0
    holding, surplus = [largest] + [least] * (number_of - 1), total - largest - least * (number_of - 1)
    while surplus > 0:
        movable = [i for i in range(1, number_of) if holding[i] < largest] or [i for i in range(1, number_of) if holding[i] < reach]
        mass, left = sum([weights[i] for i in movable]), surplus
        for i in movable:
            more = min(reach - holding[i], max(1, left * weights[i] // mass), surplus)
            holding[i] = holding[i] + more
            surplus = surplus - more
    return np.array(holding)


def bell_draw(own_key, dims, width, reach, split=(), held_as=jnp.bfloat16):
    loudness = level_of(own_key, dims, split, -0.22, 0.18) if split else 1.0
    array = jax.random.normal(own_key, dims, jnp.float32) * width * loudness
    return jnp.minimum(jnp.maximum(array, -reach), reach).astype(held_as)


def setup_inputs(seed: int = 0) -> dict:
    seeds = jax.random.split(jax.random.key(seed), 11)
    grad_output = bell_draw(seeds[0], (N_EXPERT, GROUP, D), 1.0, 6.0, ((0, 32), (2, 24)))
    router_logits = bell_draw(seeds[1], (N_EXPERT, GROUP, EXPERTS), 1.5, 8.0, ((0, 32),), jnp.float32)
    expert_ids_keys = jax.random.split(jax.random.fold_in(seeds[2], 1), N_EXPERT * GROUP // GROUP)
    expert_ids_turns = jax.random.permutation(jax.random.fold_in(seeds[2], 3), N_EXPERT * GROUP // GROUP)
    expert_ids = jax.vmap(lambda own, number: routed_block(jax.random.fold_in(seeds[2], 2), own, number, GROUP, EXPERTS, TOP, MOST, 2))(expert_ids_keys, expert_ids_turns).reshape((N_EXPERT, GROUP, TOP))
    router_input = bell_draw(seeds[3], (N_EXPERT, GROUP, D), 1.0, 6.0, ((0, 32), (1, 24)))
    router_weight = bell_draw(seeds[4], (EXPERTS, D), D ** -0.5, 0.09375, ((1, 24),))
    gate_weight = bell_draw(seeds[5], (EXPERTS, D, F), D ** -0.5, 0.09375, ((0, 32), (1, 24)))
    up_weight = bell_draw(seeds[6], (EXPERTS, D, F), D ** -0.5, 0.09375, ((0, 32), (1, 24)))
    down_weight = bell_draw(seeds[7], (EXPERTS, F, D), F ** -0.5, 0.1875, ((0, 32), (2, 24)))
    gate_saved = bell_draw(seeds[8], (EXPERTS, SLOTS, F), 1.0, 6.0, ((0, 32),))
    up_saved = bell_draw(seeds[9], (EXPERTS, SLOTS, F), 1.0, 6.0, ((0, 32),))
    return {"grad_output": grad_output, "router_logits": router_logits, "expert_ids": expert_ids, "router_input": router_input, "router_weight": router_weight, "gate_weight": gate_weight, "up_weight": up_weight, "down_weight": down_weight, "gate_saved": gate_saved, "up_saved": up_saved}


route_scale = 2.5


def expert_backward(operands):
    out_grad, weight_gate, weight_up, weight_down, saved_gate, saved_up = operands
    hidden_grad = jnp.dot(out_grad, weight_down.T, preferred_element_type=jnp.float32)
    gate_value = saved_gate.astype(jnp.float32)
    up_value = saved_up.astype(jnp.float32)
    gate_sigmoid = jax.nn.sigmoid(gate_value)
    activated = gate_value * gate_sigmoid
    hidden = lax.optimization_barrier((activated * up_value).astype(jnp.bfloat16)).astype(jnp.float32)
    gate_grad = jnp.sum(hidden * hidden_grad, axis=1)
    grad_gate = (hidden_grad * up_value * gate_sigmoid * (1.0 + gate_value * (1.0 - gate_sigmoid))).astype(jnp.bfloat16)
    grad_up = (hidden_grad * activated).astype(jnp.bfloat16)
    input_grad = jnp.dot(grad_gate, weight_gate.T, preferred_element_type=jnp.float32)
    input_grad = input_grad + jnp.dot(grad_up, weight_up.T, preferred_element_type=jnp.float32)
    return input_grad.astype(jnp.bfloat16), gate_grad


def reference(grad_output, router_logits, expert_ids, router_input, router_weight, gate_weight, up_weight, down_weight, gate_saved, up_saved):
    assign_count = GROUP * TOP
    flat_ids = expert_ids.reshape(N_EXPERT, assign_count).astype(jnp.int32)
    expert_hot = (flat_ids[:, :, None] == jnp.arange(EXPERTS, dtype=jnp.int32)[None, None, :]).astype(jnp.int32)
    earlier = (jnp.cumsum(expert_hot, axis=1) - expert_hot).astype(jnp.int32)
    ranking = jnp.sum(expert_hot * earlier, axis=2).astype(jnp.int32)
    slot_index = (jnp.arange(N_EXPERT, dtype=jnp.int32)[:, None] * MOST + ranking).astype(jnp.int32)
    owner = (jnp.arange(assign_count, dtype=jnp.int32) // TOP).astype(jnp.int32)
    routed_rows = grad_output[:, owner, :]
    dispatched = jnp.zeros((EXPERTS, SLOTS, D), jnp.bfloat16).at[flat_ids, slot_index].set(routed_rows)
    expert_input, gate_grad = lax.map(expert_backward, (dispatched, gate_weight, up_weight, down_weight, gate_saved, up_saved))
    back_rows = expert_input[flat_ids, slot_index].astype(jnp.float32).reshape(N_EXPERT, GROUP, TOP, D)
    back_gate = gate_grad[flat_ids, slot_index].astype(jnp.float32).reshape(N_EXPERT, GROUP, TOP)
    scores = jax.nn.sigmoid(router_logits)
    chosen = jnp.take_along_axis(scores, expert_ids.astype(jnp.int32), axis=2)
    chosen_total = jnp.sum(chosen, axis=2, keepdims=True)
    gates = route_scale * chosen / chosen_total
    mixed = jnp.sum(gates[:, :, :, None] * back_rows, axis=2)
    mixture = jnp.sum(back_gate * gates, axis=2, keepdims=True)
    d_chosen = (route_scale * back_gate - mixture) / chosen_total
    hot_float = expert_hot.reshape(N_EXPERT, GROUP, TOP, EXPERTS).astype(jnp.float32)
    d_scores = jnp.sum(hot_float * d_chosen[:, :, :, None], axis=2)
    logit_grad = (d_scores * scores * (1.0 - scores)).astype(jnp.bfloat16)
    router_part = jnp.einsum("qge,ed->qgd", logit_grad.astype(jnp.float32), router_weight.astype(jnp.float32))
    grad_input = (mixed + router_part).astype(jnp.bfloat16)
    grad_router = jnp.einsum("qge,qgd->ed", logit_grad.astype(jnp.float32), router_input.astype(jnp.float32))
    return grad_input, grad_router
```

```python
import functools

import jax
import jax.numpy as jnp
from jax import lax
from jax.experimental import pallas as pl
from jax.experimental.pallas import tpu as pltpu
from jax.sharding import Mesh
from jax.sharding import PartitionSpec as P

DP = ("dp_0", "dp_1")
MESH = pl.DeviceIdType.MESH
VMEM = pl.BlockSpec(memory_space=pltpu.VMEM)

route_scale = 2.5


def greet(peers):
    barrier = pltpu.get_barrier_semaphore()
    for peer in peers:
        pl.semaphore_signal(barrier, inc=1, device_id=peer, device_id_type=MESH)
    pl.semaphore_wait(barrier, len(peers))


def exchange_start(axis, count, src_ref, dst_ref, send_sem, recv_sem):
    me = lax.axis_index(axis)

    def start(k, carry):
        peer = lax.rem(me + k, count)
        pltpu.make_async_remote_copy(
            src_ref=src_ref.at[peer],
            dst_ref=dst_ref.at[me],
            send_sem=send_sem.at[k],
            recv_sem=recv_sem.at[k],
            device_id={axis: peer},
            device_id_type=MESH,
        ).start()
        return carry

    lax.fori_loop(1, count, start, 0)
    dst_ref[me] = src_ref[me]


def exchange_wait(axis, count, src_ref, dst_ref, send_sem, recv_sem):
    me = lax.axis_index(axis)

    def wait(k, carry):
        peer = lax.rem(me + k, count)
        pltpu.make_async_remote_copy(
            src_ref=src_ref.at[peer],
            dst_ref=dst_ref.at[me],
            send_sem=send_sem.at[k],
            recv_sem=recv_sem.at[k],
            device_id={axis: peer},
            device_id_type=MESH,
        ).wait()
        return carry

    lax.fori_loop(1, count, wait, 0)


def exchange_kernel(count, src_ref, dst_ref, send_sem, recv_sem):
    me = lax.axis_index("expert")
    barrier = pltpu.get_barrier_semaphore()

    def signal(k, carry):
        pl.semaphore_signal(
            barrier, inc=1, device_id={"expert": lax.rem(me + k, count)}, device_id_type=MESH
        )
        return carry

    lax.fori_loop(1, count, signal, 0)
    pl.semaphore_wait(barrier, count - 1)
    exchange_start("expert", count, src_ref, dst_ref, send_sem, recv_sem)
    exchange_wait("expert", count, src_ref, dst_ref, send_sem, recv_sem)


def exchange(blocks, collective_id):
    count = blocks.shape[0]
    return pl.pallas_call(
        functools.partial(exchange_kernel, count),
        out_shape=jax.ShapeDtypeStruct(blocks.shape, blocks.dtype),
        in_specs=[VMEM],
        out_specs=VMEM,
        scratch_shapes=[pltpu.SemaphoreType.DMA((count,)), pltpu.SemaphoreType.DMA((count,))],
        compiler_params=pltpu.CompilerParams(
            collective_id=collective_id, has_side_effects=True
        ),
    )(blocks)


def dispatch_kernel(
    count, dp_0, dp_1, src_ref, row_ref, dst_ref, got_ref, send_sem, recv_sem, row_send, row_recv
):
    me = lax.axis_index("expert")
    z, h = lax.axis_index("dp_0"), lax.axis_index("dp_1")
    dp_count = dp_0 * dp_1
    mine = z * dp_1 + h
    barrier = pltpu.get_barrier_semaphore()

    def signal(k, carry):
        pl.semaphore_signal(
            barrier, inc=1, device_id={"expert": lax.rem(me + k, count)}, device_id_type=MESH
        )
        return carry

    def signal_dp(k, carry):
        peer = lax.rem(mine + k, dp_count)
        pl.semaphore_signal(
            barrier,
            inc=1,
            device_id={"dp_0": peer // dp_1, "dp_1": lax.rem(peer, dp_1)},
            device_id_type=MESH,
        )
        return carry

    def row_copy(k):
        peer = lax.rem(mine + k, dp_count)
        return pltpu.make_async_remote_copy(
            src_ref=row_ref.at[peer],
            dst_ref=got_ref.at[mine],
            send_sem=row_send.at[k],
            recv_sem=row_recv.at[k],
            device_id={"dp_0": peer // dp_1, "dp_1": lax.rem(peer, dp_1)},
            device_id_type=MESH,
        )

    def start_row(k, carry):
        row_copy(k).start()
        return carry

    def wait_row(k, carry):
        row_copy(k).wait()
        return carry

    lax.fori_loop(1, dp_count, signal_dp, 0)
    lax.fori_loop(1, count, signal, 0)
    pl.semaphore_wait(barrier, count - 1 + dp_count - 1)
    lax.fori_loop(1, dp_count, start_row, 0)
    exchange_start("expert", count, src_ref, dst_ref, send_sem, recv_sem)
    got_ref[mine] = row_ref[mine]
    exchange_wait("expert", count, src_ref, dst_ref, send_sem, recv_sem)
    lax.fori_loop(1, dp_count, wait_row, 0)


def dispatch(blocks, rows, dp_0, dp_1, collective_id):
    count, dp_count = blocks.shape[0], rows.shape[0]
    return pl.pallas_call(
        functools.partial(dispatch_kernel, count, dp_0, dp_1),
        out_shape=(
            jax.ShapeDtypeStruct(blocks.shape, blocks.dtype),
            jax.ShapeDtypeStruct(rows.shape, rows.dtype),
        ),
        in_specs=[VMEM, VMEM],
        out_specs=(VMEM, VMEM),
        scratch_shapes=[
            pltpu.SemaphoreType.DMA((count,)),
            pltpu.SemaphoreType.DMA((count,)),
            pltpu.SemaphoreType.DMA((dp_count,)),
            pltpu.SemaphoreType.DMA((dp_count,)),
        ],
        compiler_params=pltpu.CompilerParams(
            collective_id=collective_id, has_side_effects=True
        ),
    )(blocks, rows)


def all_sum_kernel(
    ring, parts, own_ref, out_ref, send_buf, recv_buf, swap_buf, send_sem, recv_sem, swap_send, swap_recv, gsend, grecv
):
    z, h = lax.axis_index("dp_0"), lax.axis_index("dp_1")
    half = ring // 2
    rows = own_ref.shape[1] // parts
    neighbour = ({"dp_0": lax.rem(z + 1, ring)}, {"dp_0": lax.rem(z + ring - 1, ring)})
    partner = {"dp_1": 1 - h}
    greet((*neighbour, partner))

    def at(way, distance):
        step = distance if way == 0 else ring - distance
        return lax.rem(z + step, ring)

    def piece(g):
        return pl.ds(g * rows, rows)

    def runs(way, distance, g):
        if distance < half or ring % 2:
            return True
        return (g < parts // 2) == (way == 0)

    def hop(way, step, g):
        return pltpu.make_async_remote_copy(
            src_ref=send_buf.at[way, step, piece(g)],
            dst_ref=recv_buf.at[way, step, piece(g)],
            send_sem=send_sem.at[way, step, g],
            recv_sem=recv_sem.at[way, step, g],
            device_id=neighbour[way],
            device_id_type=MESH,
        )

    def swap(g):
        return pltpu.make_async_remote_copy(
            src_ref=swap_buf.at[0, piece(g)],
            dst_ref=swap_buf.at[1, piece(g)],
            send_sem=swap_send.at[g],
            recv_sem=swap_recv.at[g],
            device_id=partner,
            device_id_type=MESH,
        )

    def gather(way, step, g):
        block = at(1 - way, step) if step else z
        return pltpu.make_async_remote_copy(
            src_ref=out_ref.at[block, piece(g)],
            dst_ref=out_ref.at[block, piece(g)],
            send_sem=gsend.at[way, step, g],
            recv_sem=grecv.at[way, step, g],
            device_id=neighbour[way],
            device_id_type=MESH,
        )

    for step in range(half):
        distance = half - step
        for g in range(parts):
            for way in range(2):
                if not runs(way, distance, g):
                    continue
                value = own_ref[at(way, distance), piece(g), :]
                if step and runs(way, distance + 1, g):
                    hop(way, step - 1, g).wait_recv()
                    value = value + recv_buf[way, step - 1, piece(g), :].astype(jnp.float32)
                send_buf[way, step, piece(g), :] = value.astype(jnp.bfloat16)
                hop(way, step, g).start()
    for g in range(parts):
        value = own_ref[z, piece(g), :]
        for way in range(2):
            hop(way, half - 1, g).wait_recv()
            value = value + recv_buf[way, half - 1, piece(g), :].astype(jnp.float32)
        swap_buf[0, piece(g), :] = value.astype(jnp.bfloat16)
        swap(g).start()
    for g in range(parts):
        swap(g).wait_recv()
        total = swap_buf[0, piece(g), :].astype(jnp.float32) + swap_buf[1, piece(g), :].astype(
            jnp.float32
        )
        out_ref[z, piece(g), :] = total.astype(jnp.bfloat16)
        for way in range(2):
            gather(way, 0, g).start()
    for step in range(1, half):
        for g in range(parts):
            for way in range(2):
                gather(way, step - 1, g).wait_recv()
                if runs(way, step + 1, g):
                    gather(way, step, g).start()
    for g in range(parts):
        for way in range(2):
            if runs(way, half, g):
                gather(way, half - 1, g).wait_recv()
    for step in range(half):
        for g in range(parts):
            for way in range(2):
                if runs(way, half - step, g):
                    hop(way, step, g).wait_send()
                if runs(way, step + 1, g):
                    gather(way, step, g).wait_send()
    for g in range(parts):
        swap(g).wait_send()


def all_sum(partial, ring, parts, collective_id):
    row_total, width = partial.shape
    depth = row_total // ring
    half = ring // 2
    sems = pltpu.SemaphoreType.DMA((2, half, parts))
    total = pl.pallas_call(
        functools.partial(all_sum_kernel, ring, parts),
        out_shape=jax.ShapeDtypeStruct((ring, depth, width), jnp.bfloat16),
        in_specs=[VMEM],
        out_specs=VMEM,
        scratch_shapes=[
            pltpu.VMEM((2, half, depth, width), jnp.bfloat16),
            pltpu.VMEM((2, half, depth, width), jnp.bfloat16),
            pltpu.VMEM((2, depth, width), jnp.bfloat16),
            sems,
            sems,
            pltpu.SemaphoreType.DMA((parts,)),
            pltpu.SemaphoreType.DMA((parts,)),
            sems,
            sems,
        ],
        compiler_params=pltpu.CompilerParams(
            collective_id=collective_id, has_side_effects=True
        ),
    )(partial.reshape(ring, depth, width))
    return total.reshape(row_total, width)


def split_pair(values):
    upper = values.astype(jnp.bfloat16)
    lower = (values - upper.astype(jnp.float32)).astype(jnp.bfloat16)
    return upper, lower


def activation_backward(hidden_grad, saved_gate, saved_up):
    gate_value = saved_gate.astype(jnp.float32)
    up_value = saved_up.astype(jnp.float32)
    gate_sigmoid = jax.nn.sigmoid(gate_value)
    activated = gate_value * gate_sigmoid
    hidden = (activated * up_value).astype(jnp.bfloat16).astype(jnp.float32)
    gate_share = jnp.sum(hidden * hidden_grad, axis=1)
    gate_part = (
        hidden_grad * up_value * gate_sigmoid * (1.0 + gate_value * (1.0 - gate_sigmoid))
    ).astype(jnp.bfloat16)
    up_part = (hidden_grad * activated).astype(jnp.bfloat16)
    return (gate_part, up_part, gate_share)


def local(
    grad_output,
    router_logits,
    expert_ids,
    router_input,
    router_weight,
    gate_weight,
    up_weight,
    down_weight,
    gate_saved,
    up_saved,
):
    expert_count = lax.axis_size("expert")
    dp_0, dp_1 = lax.axis_size("dp_0"), lax.axis_size("dp_1")
    dp_count = dp_0 * dp_1
    out_rows = grad_output[0]
    group_size, feature_share = out_rows.shape
    expert_total = router_logits.shape[2]
    top_count = expert_ids.shape[2]
    local_experts, slot_count, hidden_size = gate_saved.shape
    slot_depth = slot_count // expert_count
    block_rows = local_experts * slot_depth
    block_lanes = block_rows * feature_share // 128
    assign_count = group_size * top_count
    flat_ids = expert_ids[0].reshape(assign_count)
    expert_hot = (flat_ids[:, None] == jnp.arange(expert_total, dtype=jnp.int32)[None, :]).astype(
        jnp.int32
    )
    earlier = jnp.cumsum(expert_hot, axis=0) - expert_hot
    ranking = jnp.sum(expert_hot * earlier, axis=1)
    target = flat_ids * slot_depth + ranking
    slot_place = (
        jnp.arange(expert_total * slot_depth, dtype=jnp.int32)[:, None] == target[None, :]
    ).astype(jnp.bfloat16)
    owner_hot = (
        (jnp.arange(assign_count, dtype=jnp.int32) // top_count)[:, None]
        == jnp.arange(group_size, dtype=jnp.int32)[None, :]
    ).astype(jnp.bfloat16)
    slot_token = jnp.dot(slot_place, owner_hot, preferred_element_type=jnp.float32).astype(
        jnp.bfloat16
    )
    outgoing = jnp.dot(slot_token, out_rows, preferred_element_type=jnp.float32).astype(
        jnp.bfloat16
    )
    blocks = outgoing.reshape(expert_count, block_lanes, 128)
    share_pad = -feature_share % 128
    router_rows = jnp.pad(
        jnp.swapaxes(router_input[0].reshape(-1, dp_count, feature_share), 0, 1),
        ((0, 0), (0, 0), (0, share_pad)),
    )
    incoming, grouped = dispatch(blocks, router_rows, dp_0, dp_1, 0)
    incoming = jnp.swapaxes(
        incoming.reshape(expert_count, local_experts, slot_depth, feature_share), 0, 1
    ).reshape(local_experts, slot_count, feature_share)
    grouped_input = grouped[:, :, :feature_share].reshape(group_size, feature_share)
    partial_hidden = jnp.einsum(
        "esd,efd->esf", incoming, down_weight, preferred_element_type=jnp.float32
    )
    row_total = local_experts * slot_count
    hidden_grad = all_sum(partial_hidden.reshape(row_total, hidden_size), dp_0, 2, 1)
    grad_gate, grad_up, gate_grad = activation_backward(
        hidden_grad.astype(jnp.float32),
        gate_saved.reshape(row_total, hidden_size),
        up_saved.reshape(row_total, hidden_size),
    )
    grad_gate = grad_gate.reshape(local_experts, slot_count, hidden_size)
    grad_up = grad_up.reshape(local_experts, slot_count, hidden_size)
    expert_input = jnp.einsum(
        "esf,edf->esd", grad_gate, gate_weight, preferred_element_type=jnp.float32
    )
    expert_input = expert_input + jnp.einsum(
        "esf,edf->esd", grad_up, up_weight, preferred_element_type=jnp.float32
    )
    expert_input = expert_input.astype(jnp.bfloat16)

    def by_group(values):
        split = values.reshape(local_experts, expert_count, slot_depth, *values.shape[2:])
        return jnp.swapaxes(split, 0, 1)

    upper, lower = split_pair(by_group(gate_grad.reshape(local_experts, slot_count)))
    gate_rows = jnp.pad(
        jnp.stack([upper, lower], axis=1).reshape(expert_count, 2, block_rows),
        ((0, 0), (0, 0), (0, 128 - block_rows)),
    )
    returning = jnp.concatenate(
        [by_group(expert_input).reshape(expert_count, block_lanes, 128), gate_rows], axis=1
    )
    returned = exchange(returning, 2)
    rows_back = returned[:, :block_lanes].reshape(expert_total * slot_depth, feature_share)
    gate_back = (
        returned[:, block_lanes, :block_rows].astype(jnp.float32)
        + returned[:, block_lanes + 1, :block_rows].astype(jnp.float32)
    ).reshape(expert_total * slot_depth, 1)
    picked_gate = jnp.sum(
        jnp.where(
            jnp.arange(expert_total * slot_depth, dtype=jnp.int32)[:, None] == target[None, :],
            gate_back,
            0.0,
        ),
        axis=0,
    ).reshape(group_size, top_count)
    scores = jax.nn.sigmoid(router_logits[0])
    hot_float = expert_hot.reshape(group_size, top_count, expert_total).astype(jnp.float32)
    chosen = jnp.sum(hot_float * scores[:, None, :], axis=2)
    chosen_total = jnp.sum(chosen, axis=1, keepdims=True)
    gates = route_scale * chosen / chosen_total
    mixture = jnp.sum(picked_gate * gates, axis=1, keepdims=True)
    d_chosen = (route_scale * picked_gate - mixture) / chosen_total
    d_scores = jnp.sum(hot_float * d_chosen[:, :, None], axis=1)
    logit_grad = (d_scores * scores * (1.0 - scores)).astype(jnp.bfloat16)
    router_term = jnp.einsum(
        "ge,gc->ec", logit_grad, grouped_input, preferred_element_type=jnp.float32
    )
    term_blocks = router_term.reshape(expert_count, local_experts * feature_share // 128, 128)
    grad_router = jnp.sum(exchange(term_blocks, 3), axis=0).reshape(local_experts, feature_share)
    picked_rows = jnp.dot(
        slot_place.T, rows_back, preferred_element_type=jnp.float32
    )
    mixed = jnp.sum(
        gates[:, :, None] * picked_rows.reshape(group_size, top_count, feature_share), axis=1
    )
    router_part = jnp.dot(logit_grad, router_weight, preferred_element_type=jnp.float32)
    grad_input = (mixed + router_part).astype(jnp.bfloat16)[None]
    return (grad_input, grad_router)


def solution(mesh):
    torus = Mesh(
        mesh.devices.reshape(mesh.shape["dp"] // 2, 2, mesh.shape["expert"]),
        ("dp_0", "dp_1", "expert"),
    )
    placed = (
        P("expert", None, DP),
        P("expert", None, None),
        P("expert", None, None),
        P("expert", DP, None),
        P(None, DP),
        P("expert", DP, None),
        P("expert", DP, None),
        P("expert", None, DP),
        P("expert", None, None),
        P("expert", None, None),
    )
    return jax.shard_map(
        local,
        mesh=torus,
        in_specs=placed,
        out_specs=(P("expert", None, DP), P("expert", DP)),
        check_vma=False,
    )
```

```python
import functools

import jax
import jax.numpy as jnp
from jax import lax
from jax.experimental import pallas as pl
from jax.experimental.pallas import tpu as pltpu
from jax.sharding import Mesh
from jax.sharding import PartitionSpec as P

DP = ("dp_0", "dp_1")
MESH = pl.DeviceIdType.MESH
VMEM = pl.BlockSpec(memory_space=pltpu.VMEM)
HBM = pl.BlockSpec(memory_space=pl.ANY)
F32, BF16 = jnp.float32, jnp.bfloat16
LANES = 128
TAIL = 32
PIECE = 32
CHUNK = 8

route_scale = 2.5


def iota(shape, dim):
    return lax.broadcasted_iota(jnp.int32, shape, dim)


def over(values, by):
    if by & (by - 1) == 0:
        return lax.shift_right_logical(values, jnp.full_like(values, by.bit_length() - 1))
    return lax.shift_right_logical(values * (65536 // by + 1), jnp.full_like(values, 16))


def hot_of(condition):
    return jnp.where(condition, 1.0, 0.0).astype(BF16)


def mm(a, b):
    return jnp.dot(a, b, preferred_element_type=F32)


def mm_nt(a, b):
    return lax.dot_general(a, b, (((1,), (1,)), ((), ())), preferred_element_type=F32)


def split_pair(values):
    upper = values.astype(BF16)
    return upper, (values - upper.astype(F32)).astype(BF16)


def layer_kernel(
    shape,
    rows_ref,
    ids_ref,
    logits_ref,
    router_ref,
    router_weight_ref,
    gate_hbm,
    up_hbm,
    down_hbm,
    saved_gate_hbm,
    saved_up_hbm,
    grad_input_ref,
    grad_router_ref,
    gate_w,
    up_w,
    down_w,
    saved_gate,
    saved_up,
    gate_factor,
    up_factor,
    hidden_ref,
    own_ref,
    sum_ref,
    send_buf,
    recv_buf,
    swap_buf,
    out_piece,
    in_piece,
    x_main,
    x_tail,
    part_gate,
    part_up,
    e_main,
    e_tail,
    g_upper,
    g_lower,
    back_out,
    back_in,
    mix_ref,
    got_ref,
    term_out,
    term_in,
    load_sem,
    send_sem,
    recv_sem,
    swap_send,
    swap_recv,
    gsend,
    grecv,
    piece_send,
    piece_recv,
    back_send,
    back_recv,
    term_send,
    term_recv,
    row_send,
    row_recv,
):
    count, ring, dp_1, local_experts, depth, parts = shape
    me, z, h = lax.axis_index("expert"), lax.axis_index("dp_0"), lax.axis_index("dp_1")
    dp_count = ring * dp_1
    mine = z * dp_1 + h
    tokens, experts = logits_ref.shape
    feature_share = LANES + TAIL
    half = ring // 2
    block_rows, width = own_ref.shape[1:]
    expert_rows = count * depth
    rows = block_rows // parts
    per_expert = expert_rows // block_rows
    per_device = tokens // dp_count
    gate_row = local_experts * depth + depth
    neighbour = ({"dp_0": lax.rem(z + 1, ring)}, {"dp_0": lax.rem(z + ring - 1, ring)})
    partner = {"dp_1": 1 - h}

    def loads():
        copies = []
        for n, (hbm, to) in enumerate(((down_hbm, down_w), (gate_hbm, gate_w), (up_hbm, up_w))):
            for e in range(local_experts):
                for part, (at, size, put) in enumerate(
                    ((0, LANES, 0), (LANES, TAIL, LANES + e * TAIL))
                ):
                    copies.append(
                        pltpu.make_async_copy(
                            hbm.at[e, pl.ds(at, size)],
                            to.at[e, pl.ds(put, size)],
                            load_sem.at[n * 2 * local_experts + 2 * e + part],
                        )
                    )
        last = 3 * 2 * local_experts
        copies.append(pltpu.make_async_copy(saved_gate_hbm, saved_gate, load_sem.at[last]))
        copies.append(pltpu.make_async_copy(saved_up_hbm, saved_up, load_sem.at[last + 1]))
        return copies

    load = loads()
    down_loads, late_loads, saved_loads = load[:8], load[8:24], load[24:]
    for copy in down_loads + saved_loads + late_loads:
        copy.start()

    barrier = pltpu.get_barrier_semaphore()

    def dp_peer(k):
        peer = lax.rem(mine + k, dp_count)
        return {"dp_0": peer // dp_1, "dp_1": lax.rem(peer, dp_1)}

    def greet_expert(k, carry):
        pl.semaphore_signal(
            barrier, inc=1, device_id={"expert": lax.rem(me + k, count)}, device_id_type=MESH
        )
        return carry

    def greet_dp(k, carry):
        pl.semaphore_signal(barrier, inc=1, device_id=dp_peer(k), device_id_type=MESH)
        return carry

    lax.fori_loop(1, dp_count, greet_dp, 0)
    lax.fori_loop(1, count, greet_expert, 0)

    for to in (down_w, gate_w, up_w):
        for e in range(local_experts):
            first = LANES + e * TAIL
            if e:
                to[e, LANES:first, :] = jnp.zeros((e * TAIL, width), BF16)
            if e < local_experts - 1:
                size = (local_experts - 1 - e) * TAIL
                to[e, first + TAIL : first + TAIL + size, :] = jnp.zeros((size, width), BF16)

    hot_t = jnp.zeros((experts, tokens), F32)
    for k in range(ids_ref.shape[0]):
        hot_t = hot_t + jnp.where(
            iota((experts, tokens), 0) == ids_ref[k : k + 1, :], 1.0, 0.0
        )
    earlier = hot_of(iota((tokens, tokens), 0) < iota((tokens, tokens), 1))
    ranked_t = (hot_t * (mm(hot_t.astype(BF16), earlier) + 1.0)).astype(BF16)

    main_rows = count * local_experts * depth
    row, col = iota((main_rows, experts), 0), iota((main_rows, experts), 1)
    values = mm(hot_of(over(row, depth) == col), ranked_t)
    wanted = iota((main_rows, tokens), 0)
    wanted = (wanted - over(wanted, depth) * depth + 1).astype(F32)
    piece_main = mm(hot_of(values == wanted), rows_ref[:, :LANES])
    tail_rows = count * 8
    row, col = iota((tail_rows, experts), 0), iota((tail_rows, experts), 1)
    rank_of = iota((tail_rows, tokens), 0)
    rank_of = rank_of - over(rank_of, 8) * 8
    wanted = jnp.where(rank_of < depth, rank_of + 1, depth + 1000).astype(F32)
    piece_tail = jnp.zeros((tail_rows, LANES), F32)
    for e in range(local_experts):
        values = mm(hot_of(over(row, 8) * local_experts + e == col), ranked_t)
        lanes = hot_of(iota((TAIL, LANES), 0) + e * TAIL == iota((TAIL, LANES), 1))
        placed = mm(rows_ref[:, LANES:feature_share], lanes).astype(BF16)
        piece_tail = piece_tail + mm(hot_of(values == wanted), placed)
    out_piece[...] = jnp.concatenate(
        [
            piece_main.reshape(count, local_experts * depth, LANES),
            piece_tail.reshape(count, 8, LANES),
        ],
        axis=1,
    ).astype(BF16)

    pl.semaphore_wait(barrier, count - 1 + dp_count - 1)

    def exchange(k, src, dst, send, recv):
        peer = lax.rem(me + k, count)
        return pltpu.make_async_remote_copy(
            src_ref=src.at[peer],
            dst_ref=dst.at[me],
            send_sem=send.at[k],
            recv_sem=recv.at[k],
            device_id={"expert": peer},
            device_id_type=MESH,
        )

    def start_exchange(*refs):
        def start(k, carry):
            exchange(k, *refs).start()
            return carry

        lax.fori_loop(1, count, start, 0)

    def wait_exchange(*refs):
        def wait(k, carry):
            exchange(k, *refs).wait()
            return carry

        lax.fori_loop(1, count, wait, 0)

    piece = (out_piece, in_piece, piece_send, piece_recv)
    back = (back_out, back_in, back_send, back_recv)
    term = (term_out, term_in, term_send, term_recv)
    start_exchange(*piece)
    in_piece[me] = out_piece[me]

    def window(peer):
        return pl.multiple_of(peer * feature_share // LANES * LANES, LANES)

    def row_copy(k):
        peer = lax.rem(mine + k, dp_count)
        return pltpu.make_async_remote_copy(
            src_ref=router_ref.at[:, pl.ds(window(peer), 2 * LANES)],
            dst_ref=got_ref.at[mine],
            send_sem=row_send.at[k],
            recv_sem=row_recv.at[k],
            device_id=dp_peer(k),
            device_id_type=MESH,
        )

    def start_row(k, carry):
        row_copy(k).start()
        return carry

    def wait_row(k, carry):
        row_copy(k).wait()
        return carry

    lax.fori_loop(1, dp_count, start_row, 0)
    got_ref[mine] = router_ref[:, pl.ds(window(mine), 2 * LANES)]

    same = hot_of(iota((tokens, tokens), 0) == iota((tokens, tokens), 1))
    ranked = mm_nt(same, ranked_t)
    hot = jnp.where(ranked > 0.0, 1.0, 0.0)
    scores = 1.0 / (1.0 + jnp.exp(-logits_ref[...]))
    total = jnp.sum(scores * hot, axis=1, keepdims=True)
    gates = route_scale * (scores * hot) / total
    gate_upper, gate_lower = split_pair(gates)
    ranked_b = ranked.astype(BF16)
    span = count * PIECE
    slot = iota((experts, span), 1)
    inside = slot - over(slot, PIECE) * PIECE
    named = iota((experts, span), 0)
    line = iota((tokens, span), 1)
    line = line - over(line, PIECE) * PIECE
    line_rank = line - over(line, depth) * depth
    for e in range(local_experts + 1):
        if e == local_experts:
            of_expert = over(slot, PIECE) * local_experts + over(inside, depth)
            take = inside < local_experts * depth
            wanted = jnp.where(line < local_experts * depth, line_rank + 1, depth + 1000)
        else:
            of_expert = over(slot, PIECE) * local_experts + e
            take = (inside >= local_experts * depth) & (inside < gate_row)
            wanted = jnp.where(
                (line >= local_experts * depth) & (line < gate_row), line_rank + 1, depth + 1000
            )
        spread = hot_of((of_expert == named) & take)
        holds = mm(ranked_b, spread) == wanted.astype(F32)
        for n, part in enumerate((gate_upper, gate_lower)):
            at = (2 * e + n) * tokens
            mix_ref[at : at + tokens, :] = jnp.where(holds, mm(part, spread), 0.0).astype(BF16)

    for copy in saved_loads:
        copy.wait()

    def factors(block):
        def some(n, carry):
            at = pl.ds(pl.multiple_of(n * 16, 16), 16)
            gate_value = saved_gate[block, at, :].astype(F32)
            up_value = saved_up[block, at, :].astype(F32)
            sigmoid = 1.0 / (1.0 + jnp.exp(-gate_value))
            active = gate_value * sigmoid
            hidden_ref[block, at, :] = (active * up_value).astype(BF16)
            gate_factor[block, at, :] = (
                up_value * sigmoid * (1.0 + gate_value * (1.0 - sigmoid))
            )
            up_factor[block, at, :] = active
            return carry

        lax.fori_loop(0, block_rows // 16, some, 0)

    early = max(ring - half - 2, 0)
    for block in range(early):
        factors(block)

    chunk_rows = CHUNK * depth
    order_rows = (local_experts + 1) * chunk_rows

    def source(values):
        of_expert = over(values, chunk_rows)
        within = values - of_expert * chunk_rows
        group = over(within, depth)
        return group * PIECE + of_expert * depth + within - group * depth

    order_in = hot_of(
        source(iota((order_rows, CHUNK * PIECE), 0)) == iota((order_rows, CHUNK * PIECE), 1)
    )
    for copy in down_loads:
        copy.wait()
    wait_exchange(*piece)
    for n in range(count // CHUNK):
        chunk = in_piece[n * CHUNK : (n + 1) * CHUNK].reshape(CHUNK * PIECE, LANES)
        ordered = mm(order_in, chunk).astype(BF16)
        for e in range(local_experts):
            at = e * expert_rows + n * chunk_rows
            x_main[at : at + chunk_rows, :] = ordered[e * chunk_rows : (e + 1) * chunk_rows]
        x_tail[n * chunk_rows : (n + 1) * chunk_rows, :] = ordered[local_experts * chunk_rows :]

    def at(way, distance):
        step = distance if way == 0 else ring - distance
        return lax.rem(z + step, ring)

    def part(g):
        return pl.ds(g * rows, rows)

    def runs(way, distance, g):
        if distance < half:
            return True
        return (g < parts // 2) == (way == 0)

    def hop(way, step, g):
        return pltpu.make_async_remote_copy(
            src_ref=send_buf.at[way, step, part(g)],
            dst_ref=recv_buf.at[way, step, part(g)],
            send_sem=send_sem.at[way, step, g],
            recv_sem=recv_sem.at[way, step, g],
            device_id=neighbour[way],
            device_id_type=MESH,
        )

    def swap(g):
        return pltpu.make_async_remote_copy(
            src_ref=swap_buf.at[0, part(g)],
            dst_ref=swap_buf.at[1, part(g)],
            send_sem=swap_send.at[g],
            recv_sem=swap_recv.at[g],
            device_id=partner,
            device_id_type=MESH,
        )

    def gather(way, step, g):
        block = at(1 - way, step) if step else z
        return pltpu.make_async_remote_copy(
            src_ref=sum_ref.at[block, part(g)],
            dst_ref=sum_ref.at[block, part(g)],
            send_sem=gsend.at[way, step, g],
            recv_sem=grecv.at[way, step, g],
            device_id=neighbour[way],
            device_id_type=MESH,
        )

    far = lax.rem(z + half, ring)
    far_expert = far // per_expert
    far_tail = pl.ds(pl.multiple_of(lax.rem(far, per_expert) * block_rows, block_rows), block_rows)
    far_rows = pl.ds(pl.multiple_of(far * block_rows, block_rows), block_rows)
    first = jnp.concatenate([x_main[far_rows, :], x_tail[far_tail, :]], axis=1)
    first = mm(first, down_w[far_expert]).astype(BF16)
    for way in range(2):
        for g in range(parts):
            if runs(way, half, g):
                send_buf[way, 0, part(g), :] = first[g * rows : (g + 1) * rows]
                hop(way, 0, g).start()
    for e in range(local_experts):
        inputs = jnp.concatenate(
            [x_main[e * expert_rows : (e + 1) * expert_rows, :], x_tail[...]], axis=1
        )
        terms = mm(inputs, down_w[e])
        for n in range(per_expert):
            own_ref[e * per_expert + n] = terms[n * block_rows : (n + 1) * block_rows]

    for step in range(1, half):
        distance = half - step
        for g in range(parts):
            for way in range(2):
                value = own_ref[at(way, distance), part(g), :]
                if runs(way, distance + 1, g):
                    hop(way, step - 1, g).wait_recv()
                    value = value + recv_buf[way, step - 1, part(g), :].astype(F32)
                send_buf[way, step, part(g), :] = value.astype(BF16)
                hop(way, step, g).start()
        if early + step - 1 < ring:
            factors(early + step - 1)
    for g in range(parts):
        value = own_ref[z, part(g), :]
        for way in range(2):
            if runs(way, 1, g):
                hop(way, half - 1, g).wait_recv()
                value = value + recv_buf[way, half - 1, part(g), :].astype(F32)
        own_ref[z, part(g), :] = value
        swap_buf[0, part(g), :] = value.astype(BF16)
        swap(g).start()
    for block in range(early + half - 1, ring):
        factors(block)
    for copy in late_loads:
        copy.wait()
    e_tail[...] = jnp.zeros_like(e_tail)
    for g in range(parts):
        swap(g).wait_recv()
        total_sum = own_ref[z, part(g), :] + swap_buf[1, part(g), :].astype(F32)
        sum_ref[z, part(g), :] = total_sum.astype(BF16)
        for way in range(2):
            if runs(way, 1, g):
                gather(way, 0, g).start()

    def project(block):
        of_expert = block // per_expert
        first_row = lax.rem(block, per_expert) * block_rows
        gate_rows = []
        for n in range(block_rows // 16):
            cut = slice(n * 16, (n + 1) * 16)
            value = sum_ref[block, cut, :].astype(F32)
            gate_rows.append(
                jnp.sum(hidden_ref[block, cut, :].astype(F32) * value, axis=1, keepdims=True)
            )
            part_gate[cut, :] = (value * gate_factor[block, cut, :]).astype(BF16)
            part_up[cut, :] = (value * up_factor[block, cut, :]).astype(BF16)
        gate_sum = jnp.concatenate(gate_rows, axis=0)
        out = mm_nt(part_gate[...], gate_w[of_expert]) + mm_nt(part_up[...], up_w[of_expert])
        block_at = pl.ds(pl.multiple_of(block * block_rows, block_rows), block_rows)
        tail_at = pl.ds(pl.multiple_of(first_row, block_rows), block_rows)
        e_main[block_at, :] = out[:, :LANES].astype(BF16)
        e_tail[tail_at, :] = e_tail[tail_at, :] + out[:, LANES:]
        place = iota((block_rows, LANES), 0) + first_row
        place = place - over(place, depth) * depth + of_expert * depth
        held = place == iota((block_rows, LANES), 1)
        upper, lower = split_pair(jnp.broadcast_to(gate_sum, (block_rows, LANES)))
        zero = jnp.zeros((block_rows, LANES), F32)
        g_upper[block_at, :] = jnp.where(held, upper.astype(F32), zero).astype(BF16)
        g_lower[block_at, :] = jnp.where(held, lower.astype(F32), zero).astype(BF16)

    project(z)
    for step in range(1, half):
        for g in range(parts):
            for way in range(2):
                gather(way, step - 1, g).wait_recv()
                if runs(way, step + 1, g):
                    gather(way, step, g).start()

        def arrived(way, carry):
            project(lax.rem(z + jnp.where(way == 0, ring - step, step), ring))
            return carry

        lax.fori_loop(0, 2, arrived, 0)
    for g in range(parts):
        for way in range(2):
            if runs(way, half, g):
                gather(way, half - 1, g).wait_recv()
    project(far)

    piece_of = iota((CHUNK * PIECE, order_rows), 0)
    order_out = hot_of(source(iota((CHUNK * PIECE, order_rows), 1)) == piece_of)
    gate_cols = local_experts * chunk_rows
    group_of = iota((CHUNK * PIECE, gate_cols), 1)
    group_of = over(group_of - over(group_of, chunk_rows) * chunk_rows, depth) * PIECE
    piece_of = iota((CHUNK * PIECE, gate_cols), 0)
    order_upper = hot_of(group_of + gate_row == piece_of)
    order_lower = hot_of(group_of + gate_row + 1 == piece_of)
    for n in range(count // CHUNK):

        def cut(ref):
            return [
                ref[e * expert_rows + n * chunk_rows : e * expert_rows + (n + 1) * chunk_rows, :]
                for e in range(local_experts)
            ]

        tail = e_tail[n * chunk_rows : (n + 1) * chunk_rows, :].astype(BF16)
        pieces = mm(order_out, jnp.concatenate([*cut(e_main), tail], axis=0))
        pieces = pieces + mm(order_upper, jnp.concatenate(cut(g_upper), axis=0))
        pieces = pieces + mm(order_lower, jnp.concatenate(cut(g_lower), axis=0))
        back_out[n * CHUNK : (n + 1) * CHUNK] = pieces.astype(BF16).reshape(CHUNK, PIECE, LANES)
    start_exchange(*back)
    back_in[me] = back_out[me]

    gate_lines = iota((count, span), 1) - iota((count, span), 0) * PIECE
    pick_lines = hot_of((gate_lines == gate_row) | (gate_lines == gate_row + 1))
    lane, to = iota((LANES, depth * experts), 0), iota((LANES, depth * experts), 1)
    to_rank = over(to, experts)
    to_expert = to - to_rank * experts
    to_local = to_expert - over(to_expert, local_experts) * local_experts
    to_lane = hot_of(lane == to_local * depth + to_rank)
    to = iota((count, depth * experts), 1)
    to_expert = to - over(to, experts) * experts
    from_owner = over(to_expert, local_experts) == iota((count, depth * experts), 0)
    line8 = iota((count * 8, experts), 0)
    owner8 = over(line8, 8)
    inner8 = line8 - owner8 * 8
    inner8 = inner8 - over(inner8, local_experts) * local_experts
    repeat8 = hot_of(owner8 * local_experts + inner8 == iota((count * 8, experts), 1))
    token8 = iota((tokens, dp_count * 8), 1)
    inner = token8 - over(token8, 8) * 8
    widen = hot_of(
        (over(token8, 8) * per_device + inner == iota((tokens, dp_count * 8), 0))
        & (inner < per_device)
    )
    lax.fori_loop(1, dp_count, wait_row, 0)
    grouped = got_ref[...].astype(F32).reshape(dp_count * 8, 2 * LANES).astype(BF16)

    wait_exchange(*back)
    landed = back_in[...].reshape(span, LANES)
    lines_upper, lines_lower = split_pair(mm(pick_lines, landed))
    by_rank = mm(lines_upper, to_lane) + mm(lines_lower, to_lane)
    by_rank = jnp.sum(jnp.where(from_owner, by_rank, 0.0), axis=0, keepdims=True)
    picked = jnp.zeros((tokens, experts), F32)
    for r in range(depth):
        picked = picked + jnp.where(
            ranked == float(r + 1), by_rank[:, r * experts : (r + 1) * experts], 0.0
        )
    mixture = jnp.sum(picked * gates, axis=1, keepdims=True)
    d_chosen = hot * (route_scale * picked - mixture) / total
    logit_grad = (d_chosen * scores * (1.0 - scores)).astype(BF16)
    spread8 = mm(mm_nt(repeat8, logit_grad).astype(BF16), widen).astype(BF16)
    terms = mm(spread8, grouped)
    shift = lax.rem(mine * feature_share, LANES)
    terms = pltpu.roll(terms, lax.rem(2 * LANES - shift, 2 * LANES), 1)
    line8 = iota((count * 8, LANES), 0)
    line8 = line8 - over(line8, 8) * 8
    term_out[...] = jnp.where(
        line8 < local_experts, terms[:, :LANES], terms[:, LANES:]
    ).reshape(count, 8, LANES)
    start_exchange(*term)
    term_in[me] = term_out[me]

    mixed = mm(mix_ref[...], landed)
    lane_of = over(iota((tokens, LANES), 1), TAIL)
    tails = jnp.zeros((tokens, LANES), F32)
    for e in range(local_experts):
        at_row = 2 * e * tokens
        both = mixed[at_row : at_row + tokens] + mixed[at_row + tokens : at_row + 2 * tokens]
        tails = tails + jnp.where(lane_of == e, both, 0.0)
    folded = tails
    for e in range(1, local_experts):
        folded = folded + pltpu.roll(tails, LANES - e * TAIL, 1)
    at_row = 2 * local_experts * tokens
    main = mixed[at_row : at_row + tokens] + mixed[at_row + tokens : at_row + 2 * tokens]
    main = main + mm_nt(logit_grad, router_weight_ref[:LANES, :])
    side = folded[:, :TAIL] + mm_nt(logit_grad, router_weight_ref[LANES:feature_share, :])
    grad_input_ref[:, :LANES] = main.astype(BF16)
    grad_input_ref[:, LANES:feature_share] = side.astype(BF16)

    for step in range(half):
        for g in range(parts):
            for way in range(2):
                if runs(way, half - step, g):
                    hop(way, step, g).wait_send()
                if runs(way, step + 1, g):
                    gather(way, step, g).wait_send()
    for g in range(parts):
        swap(g).wait_send()

    wait_exchange(*term)
    sums = jnp.sum(term_in[...], axis=0)
    grad_router_ref[:, :LANES] = sums[:local_experts]
    grad_router_ref[:, LANES:feature_share] = sums[local_experts : 2 * local_experts, :TAIL]


def local(
    grad_output,
    router_logits,
    expert_ids,
    router_input,
    router_weight,
    gate_weight,
    up_weight,
    down_weight,
    gate_saved,
    up_saved,
):
    count = lax.axis_size("expert")
    ring, dp_1 = lax.axis_size("dp_0"), lax.axis_size("dp_1")
    dp_count = ring * dp_1
    tokens, feature_share = grad_output.shape[1:]
    experts = router_logits.shape[2]
    local_experts, slot_count, width = gate_saved.shape
    depth = slot_count // count
    expert_rows = slot_count
    row_total = local_experts * slot_count
    block_rows = row_total // ring
    parts = block_rows // 16
    half = ring // 2
    span = count * PIECE
    blocked = (ring, block_rows, width)
    hops = pltpu.SemaphoreType.DMA((2, half, parts))
    swaps = pltpu.SemaphoreType.DMA((parts,))
    peers = pltpu.SemaphoreType.DMA((count,))
    dp_peers = pltpu.SemaphoreType.DMA((dp_count,))
    router_rows = jnp.pad(router_input[0], ((0, 8 - tokens // dp_count), (0, 0)))
    grad_input, grad_router = pl.pallas_call(
        functools.partial(layer_kernel, (count, ring, dp_1, local_experts, depth, parts)),
        out_shape=(
            jax.ShapeDtypeStruct((tokens, feature_share), BF16),
            jax.ShapeDtypeStruct((local_experts, feature_share), F32),
        ),
        in_specs=[VMEM] * 5 + [HBM] * 5,
        out_specs=(VMEM, VMEM),
        scratch_shapes=[
            pltpu.VMEM((local_experts, 2 * LANES, width), BF16),
            pltpu.VMEM((local_experts, 2 * LANES, width), BF16),
            pltpu.VMEM((local_experts, 2 * LANES, width), BF16),
            pltpu.VMEM(blocked, BF16),
            pltpu.VMEM(blocked, BF16),
            pltpu.VMEM(blocked, F32),
            pltpu.VMEM(blocked, F32),
            pltpu.VMEM(blocked, BF16),
            pltpu.VMEM(blocked, F32),
            pltpu.VMEM(blocked, BF16),
            pltpu.VMEM((2, half, block_rows, width), BF16),
            pltpu.VMEM((2, half, block_rows, width), BF16),
            pltpu.VMEM((2, block_rows, width), BF16),
            pltpu.VMEM((count, PIECE, LANES), BF16),
            pltpu.VMEM((count, PIECE, LANES), BF16),
            pltpu.VMEM((row_total, LANES), BF16),
            pltpu.VMEM((expert_rows, LANES), BF16),
            pltpu.VMEM((block_rows, width), BF16),
            pltpu.VMEM((block_rows, width), BF16),
            pltpu.VMEM((row_total, LANES), BF16),
            pltpu.VMEM((expert_rows, LANES), F32),
            pltpu.VMEM((row_total, LANES), BF16),
            pltpu.VMEM((row_total, LANES), BF16),
            pltpu.VMEM((count, PIECE, LANES), BF16),
            pltpu.VMEM((count, PIECE, LANES), BF16),
            pltpu.VMEM(((local_experts + 1) * 2 * tokens, span), BF16),
            pltpu.VMEM((dp_count, 8, 2 * LANES), BF16),
            pltpu.VMEM((count, 8, LANES), F32),
            pltpu.VMEM((count, 8, LANES), F32),
            pltpu.SemaphoreType.DMA((3 * 2 * local_experts + 2,)),
            hops,
            hops,
            swaps,
            swaps,
            hops,
            hops,
            peers,
            peers,
            peers,
            peers,
            peers,
            peers,
            dp_peers,
            dp_peers,
        ],
        compiler_params=pltpu.CompilerParams(
            collective_id=0, has_side_effects=True, vmem_limit_bytes=60 << 20
        ),
    )(
        grad_output[0],
        expert_ids[0].T,
        router_logits[0],
        router_rows,
        router_weight.T,
        gate_weight,
        up_weight,
        jnp.swapaxes(down_weight, 1, 2),
        gate_saved.reshape(blocked),
        up_saved.reshape(blocked),
    )
    return (grad_input[None], grad_router)


def solution(mesh):
    torus = Mesh(
        mesh.devices.reshape(mesh.shape["dp"] // 2, 2, mesh.shape["expert"]),
        ("dp_0", "dp_1", "expert"),
    )
    placed = (
        P("expert", None, DP),
        P("expert", None, None),
        P("expert", None, None),
        P("expert", DP, None),
        P(None, DP),
        P("expert", DP, None),
        P("expert", DP, None),
        P("expert", None, DP),
        P("expert", None, None),
        P("expert", None, None),
    )
    return jax.shard_map(
        local,
        mesh=torus,
        in_specs=placed,
        out_specs=(P("expert", None, DP), P("expert", DP)),
        check_vma=False,
    )
```

```python
import functools

import jax
import jax.numpy as jnp
from jax import lax
from jax.experimental import pallas as pl
from jax.experimental.pallas import tpu as pltpu
from jax.sharding import Mesh
from jax.sharding import PartitionSpec as P

DP = ("dp_0", "dp_1")
MESH = pl.DeviceIdType.MESH
VMEM = pl.BlockSpec(memory_space=pltpu.VMEM)
HBM = pl.BlockSpec(memory_space=pl.ANY)
F32, BF16 = jnp.float32, jnp.bfloat16
LANES = 128
TAIL = 32
PIECE = 32
CHUNK = 8

route_scale = 2.5


def iota(shape, dim):
    return lax.broadcasted_iota(jnp.int32, shape, dim)


def over(values, by):
    if by & (by - 1) == 0:
        return lax.shift_right_logical(values, jnp.full_like(values, by.bit_length() - 1))
    return lax.shift_right_logical(values * (65536 // by + 1), jnp.full_like(values, 16))


def hot_of(condition):
    return jnp.where(condition, 1.0, 0.0).astype(BF16)


def mm(a, b):
    return jnp.dot(a, b, preferred_element_type=F32)


def mm_nt(a, b):
    return lax.dot_general(a, b, (((1,), (1,)), ((), ())), preferred_element_type=F32)


def split_pair(values):
    upper = values.astype(BF16)
    return upper, (values - upper.astype(F32)).astype(BF16)


def layer_kernel(
    shape,
    rows_hbm,
    ids_hbm,
    logits_hbm,
    router_hbm,
    router_weight_hbm,
    gate_hbm,
    up_hbm,
    down_hbm,
    saved_gate_hbm,
    saved_up_hbm,
    grad_input_ref,
    grad_router_ref,
    rows_ref,
    ids_ref,
    logits_ref,
    router_in,
    router_weight_ref,
    router_ref,
    gate_w,
    up_w,
    down_w,
    saved_gate,
    saved_up,
    gate_factor,
    up_factor,
    hidden_ref,
    own_ref,
    sum_ref,
    send_buf,
    recv_buf,
    swap_buf,
    out_piece,
    in_piece,
    x_main,
    x_tail,
    part_gate,
    part_up,
    e_main,
    e_tail,
    g_upper,
    g_lower,
    gate_out,
    gate_in,
    back_out,
    back_in,
    mix_ref,
    got_ref,
    term_out,
    term_in,
    small_sem,
    load_sem,
    send_sem,
    recv_sem,
    swap_send,
    swap_recv,
    gsend,
    grecv,
    piece_send,
    piece_recv,
    gate_send,
    gate_recv,
    back_send,
    back_recv,
    term_send,
    term_recv,
    row_send,
    row_recv,
):
    count, ring, dp_1, local_experts, depth, parts = shape
    me, z, h = lax.axis_index("expert"), lax.axis_index("dp_0"), lax.axis_index("dp_1")
    dp_count = ring * dp_1
    mine = z * dp_1 + h
    tokens, experts = logits_hbm.shape
    feature_share = LANES + TAIL
    half = ring // 2
    block_rows, width = own_ref.shape[1:]
    expert_rows = count * depth
    rows = block_rows // parts
    per_expert = expert_rows // block_rows
    per_device = tokens // dp_count
    gate_row = local_experts * depth + depth
    neighbour = ({"dp_0": lax.rem(z + 1, ring)}, {"dp_0": lax.rem(z + ring - 1, ring)})
    partner = {"dp_1": 1 - h}

    def loads():
        copies = []
        for n, (hbm, to) in enumerate(((down_hbm, down_w), (gate_hbm, gate_w), (up_hbm, up_w))):
            for e in range(local_experts):
                for part, (at, size, put) in enumerate(
                    ((0, LANES, 0), (LANES, TAIL, LANES + e * TAIL))
                ):
                    copies.append(
                        pltpu.make_async_copy(
                            hbm.at[e, pl.ds(at, size)],
                            to.at[e, pl.ds(put, size)],
                            load_sem.at[n * 2 * local_experts + 2 * e + part],
                        )
                    )
        last = 3 * 2 * local_experts
        copies.append(pltpu.make_async_copy(saved_gate_hbm, saved_gate, load_sem.at[last]))
        copies.append(pltpu.make_async_copy(saved_up_hbm, saved_up, load_sem.at[last + 1]))
        return copies

    small = [
        pltpu.make_async_copy(hbm, to, small_sem.at[n])
        for n, (hbm, to) in enumerate(
            (
                (ids_hbm, ids_ref),
                (rows_hbm, rows_ref),
                (router_hbm, router_in),
                (logits_hbm, logits_ref),
                (router_weight_hbm, router_weight_ref),
            )
        )
    ]
    for copy in small:
        copy.start()

    barrier = pltpu.get_barrier_semaphore()

    def dp_peer(k):
        peer = lax.rem(mine + k, dp_count)
        return {"dp_0": peer // dp_1, "dp_1": lax.rem(peer, dp_1)}

    def greet_expert(k, carry):
        pl.semaphore_signal(
            barrier, inc=1, device_id={"expert": lax.rem(me + k, count)}, device_id_type=MESH
        )
        return carry

    def greet_dp(k, carry):
        pl.semaphore_signal(barrier, inc=1, device_id=dp_peer(k), device_id_type=MESH)
        return carry

    lax.fori_loop(1, dp_count, greet_dp, 0)
    lax.fori_loop(1, count, greet_expert, 0)
    load = loads()
    down_loads, late_loads, saved_loads = load[:8], load[8:24], load[24:]
    for copy in down_loads + saved_loads + late_loads:
        copy.start()

    small[0].wait()
    hot_t = jnp.zeros((experts, tokens), F32)
    for k in range(ids_ref.shape[0]):
        hot_t = hot_t + jnp.where(
            iota((experts, tokens), 0) == ids_ref[k : k + 1, :], 1.0, 0.0
        )
    earlier = hot_of(iota((tokens, tokens), 0) < iota((tokens, tokens), 1))
    ranked_t = (hot_t * (mm(hot_t.astype(BF16), earlier) + 1.0)).astype(BF16)

    main_rows = count * local_experts * depth
    row, col = iota((main_rows, experts), 0), iota((main_rows, experts), 1)
    values = mm(hot_of(over(row, depth) == col), ranked_t)
    wanted = iota((main_rows, tokens), 0)
    wanted = (wanted - over(wanted, depth) * depth + 1).astype(F32)
    small[1].wait()
    piece_main = mm(hot_of(values == wanted), rows_ref[:, :LANES])
    tail_rows = count * 8
    row, col = iota((tail_rows, experts), 0), iota((tail_rows, experts), 1)
    rank_of = iota((tail_rows, tokens), 0)
    rank_of = rank_of - over(rank_of, 8) * 8
    wanted = jnp.where(rank_of < depth, rank_of + 1, depth + 1000).astype(F32)
    piece_tail = jnp.zeros((tail_rows, LANES), F32)
    for e in range(local_experts):
        values = mm(hot_of(over(row, 8) * local_experts + e == col), ranked_t)
        lanes = hot_of(iota((TAIL, LANES), 0) + e * TAIL == iota((TAIL, LANES), 1))
        placed = mm(rows_ref[:, LANES:feature_share], lanes).astype(BF16)
        piece_tail = piece_tail + mm(hot_of(values == wanted), placed)
    out_piece[...] = jnp.concatenate(
        [
            piece_main.reshape(count, local_experts * depth, LANES),
            piece_tail.reshape(count, 8, LANES),
        ],
        axis=1,
    ).astype(BF16)

    small[2].wait()
    router_ref[...] = jnp.concatenate(
        [
            router_in[...].astype(F32),
            jnp.zeros((8 - per_device, router_in.shape[1]), F32),
        ],
        axis=0,
    ).astype(BF16)

    pl.semaphore_wait(barrier, count - 1 + dp_count - 1)

    def exchange(k, src, dst, send, recv):
        peer = lax.rem(me + k, count)
        return pltpu.make_async_remote_copy(
            src_ref=src.at[peer],
            dst_ref=dst.at[me],
            send_sem=send.at[k],
            recv_sem=recv.at[k],
            device_id={"expert": peer},
            device_id_type=MESH,
        )

    def start_exchange(*refs):
        def start(k, carry):
            exchange(k, *refs).start()
            return carry

        lax.fori_loop(1, count, start, 0)

    def wait_exchange(*refs):
        def wait(k, carry):
            exchange(k, *refs).wait()
            return carry

        lax.fori_loop(1, count, wait, 0)

    piece = (out_piece, in_piece, piece_send, piece_recv)
    early_gate = (gate_out, gate_in, gate_send, gate_recv)
    back = (back_out, back_in, back_send, back_recv)
    term = (term_out, term_in, term_send, term_recv)
    start_exchange(*piece)
    in_piece[me] = out_piece[me]

    def window(peer):
        return pl.multiple_of(peer * feature_share // LANES * LANES, LANES)

    def row_copy(k):
        peer = lax.rem(mine + k, dp_count)
        return pltpu.make_async_remote_copy(
            src_ref=router_ref.at[:, pl.ds(window(peer), 2 * LANES)],
            dst_ref=got_ref.at[mine],
            send_sem=row_send.at[k],
            recv_sem=row_recv.at[k],
            device_id=dp_peer(k),
            device_id_type=MESH,
        )

    def start_row(k, carry):
        row_copy(k).start()
        return carry

    def wait_row(k, carry):
        row_copy(k).wait()
        return carry

    lax.fori_loop(1, dp_count, start_row, 0)
    got_ref[mine] = router_ref[:, pl.ds(window(mine), 2 * LANES)]

    for copy in small[3:]:
        copy.wait()
    for to in (down_w, gate_w, up_w):
        for e in range(local_experts):
            first = LANES + e * TAIL
            if e:
                to[e, LANES:first, :] = jnp.zeros((e * TAIL, width), BF16)
            if e < local_experts - 1:
                size = (local_experts - 1 - e) * TAIL
                to[e, first + TAIL : first + TAIL + size, :] = jnp.zeros((size, width), BF16)

    same = hot_of(iota((tokens, tokens), 0) == iota((tokens, tokens), 1))
    ranked = mm_nt(same, ranked_t)
    hot = jnp.where(ranked > 0.0, 1.0, 0.0)
    scores = 1.0 / (1.0 + jnp.exp(-logits_ref[...]))
    total = jnp.sum(scores * hot, axis=1, keepdims=True)
    gates = route_scale * (scores * hot) / total
    gate_upper, gate_lower = split_pair(gates)
    ranked_b = ranked.astype(BF16)
    span = count * PIECE
    slot = iota((experts, span), 1)
    inside = slot - over(slot, PIECE) * PIECE
    named = iota((experts, span), 0)
    line = iota((tokens, span), 1)
    line = line - over(line, PIECE) * PIECE
    line_rank = line - over(line, depth) * depth
    for e in range(local_experts + 1):
        if e == local_experts:
            of_expert = over(slot, PIECE) * local_experts + over(inside, depth)
            take = inside < local_experts * depth
            wanted = jnp.where(line < local_experts * depth, line_rank + 1, depth + 1000)
        else:
            of_expert = over(slot, PIECE) * local_experts + e
            take = (inside >= local_experts * depth) & (inside < gate_row)
            wanted = jnp.where(
                (line >= local_experts * depth) & (line < gate_row), line_rank + 1, depth + 1000
            )
        spread = hot_of((of_expert == named) & take)
        holds = mm(ranked_b, spread) == wanted.astype(F32)
        for n, part in enumerate((gate_upper, gate_lower)):
            at = (2 * e + n) * tokens
            mix_ref[at : at + tokens, :] = jnp.where(holds, mm(part, spread), 0.0).astype(BF16)

    for copy in saved_loads:
        copy.wait()

    def factors(block):
        def some(n, carry):
            at = pl.ds(pl.multiple_of(n * 16, 16), 16)
            gate_value = saved_gate[block, at, :].astype(F32)
            up_value = saved_up[block, at, :].astype(F32)
            sigmoid = 1.0 / (1.0 + jnp.exp(-gate_value))
            active = gate_value * sigmoid
            hidden_ref[block, at, :] = (active * up_value).astype(BF16)
            gate_factor[block, at, :] = (
                up_value * sigmoid * (1.0 + gate_value * (1.0 - sigmoid))
            )
            up_factor[block, at, :] = active
            return carry

        lax.fori_loop(0, block_rows // 16, some, 0)

    early = max(ring - half - 2, 0)
    for block in range(early):
        factors(block)

    chunk_rows = CHUNK * depth
    order_rows = (local_experts + 1) * chunk_rows

    def source(values):
        of_expert = over(values, chunk_rows)
        within = values - of_expert * chunk_rows
        group = over(within, depth)
        return group * PIECE + of_expert * depth + within - group * depth

    order_in = hot_of(
        source(iota((order_rows, CHUNK * PIECE), 0)) == iota((order_rows, CHUNK * PIECE), 1)
    )
    for copy in down_loads:
        copy.wait()
    wait_exchange(*piece)
    for n in range(count // CHUNK):
        chunk = in_piece[n * CHUNK : (n + 1) * CHUNK].reshape(CHUNK * PIECE, LANES)
        ordered = mm(order_in, chunk).astype(BF16)
        for e in range(local_experts):
            at = e * expert_rows + n * chunk_rows
            x_main[at : at + chunk_rows, :] = ordered[e * chunk_rows : (e + 1) * chunk_rows]
        x_tail[n * chunk_rows : (n + 1) * chunk_rows, :] = ordered[local_experts * chunk_rows :]

    def at(way, distance):
        step = distance if way == 0 else ring - distance
        return lax.rem(z + step, ring)

    def part(g):
        return pl.ds(g * rows, rows)

    def runs(way, distance, g):
        if distance < half:
            return True
        return (g < parts // 2) == (way == 0)

    def hop(way, step, g):
        return pltpu.make_async_remote_copy(
            src_ref=send_buf.at[way, step, part(g)],
            dst_ref=recv_buf.at[way, step, part(g)],
            send_sem=send_sem.at[way, step, g],
            recv_sem=recv_sem.at[way, step, g],
            device_id=neighbour[way],
            device_id_type=MESH,
        )

    def swap(g):
        return pltpu.make_async_remote_copy(
            src_ref=swap_buf.at[0, part(g)],
            dst_ref=swap_buf.at[1, part(g)],
            send_sem=swap_send.at[g],
            recv_sem=swap_recv.at[g],
            device_id=partner,
            device_id_type=MESH,
        )

    def gather(way, step, g):
        block = at(1 - way, step) if step else z
        return pltpu.make_async_remote_copy(
            src_ref=sum_ref.at[block, part(g)],
            dst_ref=sum_ref.at[block, part(g)],
            send_sem=gsend.at[way, step, g],
            recv_sem=grecv.at[way, step, g],
            device_id=neighbour[way],
            device_id_type=MESH,
        )

    far = lax.rem(z + half, ring)
    far_expert = far // per_expert
    far_tail = pl.ds(pl.multiple_of(lax.rem(far, per_expert) * block_rows, block_rows), block_rows)
    far_rows = pl.ds(pl.multiple_of(far * block_rows, block_rows), block_rows)
    first = jnp.concatenate([x_main[far_rows, :], x_tail[far_tail, :]], axis=1)
    first = mm(first, down_w[far_expert]).astype(BF16)
    for way in range(2):
        for g in range(parts):
            if runs(way, half, g):
                send_buf[way, 0, part(g), :] = first[g * rows : (g + 1) * rows]
                hop(way, 0, g).start()
    for e in range(local_experts):
        inputs = jnp.concatenate(
            [x_main[e * expert_rows : (e + 1) * expert_rows, :], x_tail[...]], axis=1
        )
        terms = mm(inputs, down_w[e])
        for n in range(per_expert):
            own_ref[e * per_expert + n] = terms[n * block_rows : (n + 1) * block_rows]

    for step in range(1, half):
        distance = half - step
        for g in range(parts):
            for way in range(2):
                value = own_ref[at(way, distance), part(g), :]
                if runs(way, distance + 1, g):
                    hop(way, step - 1, g).wait_recv()
                    value = value + recv_buf[way, step - 1, part(g), :].astype(F32)
                send_buf[way, step, part(g), :] = value.astype(BF16)
                hop(way, step, g).start()
        if early + step - 1 < ring:
            factors(early + step - 1)
    for g in range(parts):
        value = own_ref[z, part(g), :]
        for way in range(2):
            if runs(way, 1, g):
                hop(way, half - 1, g).wait_recv()
                value = value + recv_buf[way, half - 1, part(g), :].astype(F32)
        own_ref[z, part(g), :] = value
        swap_buf[0, part(g), :] = value.astype(BF16)
        swap(g).start()
    for block in range(early + half - 1, ring):
        factors(block)
    for copy in late_loads:
        copy.wait()
    e_tail[...] = jnp.zeros_like(e_tail)
    for g in range(parts):
        swap(g).wait_recv()
        total_sum = own_ref[z, part(g), :] + swap_buf[1, part(g), :].astype(F32)
        sum_ref[z, part(g), :] = total_sum.astype(BF16)
        for way in range(2):
            if runs(way, 1, g):
                gather(way, 0, g).start()

    def activate(block):
        of_expert = block // per_expert
        first_row = lax.rem(block, per_expert) * block_rows
        gate_rows = []
        for n in range(block_rows // 16):
            cut = slice(n * 16, (n + 1) * 16)
            value = sum_ref[block, cut, :].astype(F32)
            gate_rows.append(
                jnp.sum(hidden_ref[block, cut, :].astype(F32) * value, axis=1, keepdims=True)
            )
            part_gate[cut, :] = (value * gate_factor[block, cut, :]).astype(BF16)
            part_up[cut, :] = (value * up_factor[block, cut, :]).astype(BF16)
        gate_sum = jnp.concatenate(gate_rows, axis=0)
        block_at = pl.ds(pl.multiple_of(block * block_rows, block_rows), block_rows)
        place = iota((block_rows, LANES), 0) + first_row
        place = place - over(place, depth) * depth + of_expert * depth
        held = place == iota((block_rows, LANES), 1)
        upper, lower = split_pair(jnp.broadcast_to(gate_sum, (block_rows, LANES)))
        zero = jnp.zeros((block_rows, LANES), F32)
        g_upper[block_at, :] = jnp.where(held, upper.astype(F32), zero).astype(BF16)
        g_lower[block_at, :] = jnp.where(held, lower.astype(F32), zero).astype(BF16)

    def multiply(block):
        of_expert = block // per_expert
        first_row = lax.rem(block, per_expert) * block_rows
        out = mm_nt(part_gate[...], gate_w[of_expert]) + mm_nt(part_up[...], up_w[of_expert])
        block_at = pl.ds(pl.multiple_of(block * block_rows, block_rows), block_rows)
        tail_at = pl.ds(pl.multiple_of(first_row, block_rows), block_rows)
        e_main[block_at, :] = out[:, :LANES].astype(BF16)
        e_tail[tail_at, :] = e_tail[tail_at, :] + out[:, LANES:]

    def project(block):
        activate(block)
        multiply(block)

    waiting = [z]
    for step in range(1, half):
        for g in range(parts):
            for way in range(2):
                gather(way, step - 1, g).wait_recv()
                if runs(way, step + 1, g):
                    gather(way, step, g).start()
            if g in (parts // 2 - 1, parts - 1) and waiting:
                project(waiting.pop(0))
        waiting += [at(1, step), at(0, step)]
    for block in waiting:
        project(block)

    chunk_lines = CHUNK * 8
    gate_cols = local_experts * chunk_rows
    group_of = iota((chunk_lines, gate_cols), 1)
    group_of = over(group_of - over(group_of, chunk_rows) * chunk_rows, depth) * 8
    line_of = iota((chunk_lines, gate_cols), 0)
    order_upper = hot_of(group_of == line_of)
    order_lower = hot_of(group_of + 1 == line_of)
    piece_of = iota((CHUNK * PIECE, order_rows), 0)
    order_out = hot_of(source(iota((CHUNK * PIECE, order_rows), 1)) == piece_of)

    def cut_of(ref, n):
        return [
            ref[e * expert_rows + n * chunk_rows : e * expert_rows + (n + 1) * chunk_rows, :]
            for e in range(local_experts)
        ]

    for g in range(parts):
        for way in range(2):
            if runs(way, half, g):
                gather(way, half - 1, g).wait_recv()
    activate(far)
    for n in range(count // CHUNK):
        lines = mm(order_upper, jnp.concatenate(cut_of(g_upper, n), axis=0))
        lines = lines + mm(order_lower, jnp.concatenate(cut_of(g_lower, n), axis=0))
        gate_out[n * CHUNK : (n + 1) * CHUNK] = lines.reshape(CHUNK, 8, LANES).astype(BF16)
    start_exchange(*early_gate)
    gate_in[me] = gate_out[me]
    multiply(far)
    for n in range(count // CHUNK):
        tail = e_tail[n * chunk_rows : (n + 1) * chunk_rows, :].astype(BF16)
        pieces = mm(order_out, jnp.concatenate([*cut_of(e_main, n), tail], axis=0))
        back_out[n * CHUNK : (n + 1) * CHUNK] = pieces.astype(BF16).reshape(CHUNK, PIECE, LANES)
    start_exchange(*back)
    back_in[me] = back_out[me]

    gate_lines = iota((count, count * 8), 1) - iota((count, count * 8), 0) * 8
    pick_lines = hot_of((gate_lines == 0) | (gate_lines == 1))
    lane, to = iota((LANES, depth * experts), 0), iota((LANES, depth * experts), 1)
    to_rank = over(to, experts)
    to_expert = to - to_rank * experts
    to_local = to_expert - over(to_expert, local_experts) * local_experts
    to_lane = hot_of(lane == to_local * depth + to_rank)
    to = iota((count, depth * experts), 1)
    to_expert = to - over(to, experts) * experts
    from_owner = over(to_expert, local_experts) == iota((count, depth * experts), 0)
    line8 = iota((count * 8, experts), 0)
    owner8 = over(line8, 8)
    inner8 = line8 - owner8 * 8
    inner8 = inner8 - over(inner8, local_experts) * local_experts
    repeat8 = hot_of(owner8 * local_experts + inner8 == iota((count * 8, experts), 1))
    token8 = iota((tokens, dp_count * 8), 1)
    inner = token8 - over(token8, 8) * 8
    widen = hot_of(
        (over(token8, 8) * per_device + inner == iota((tokens, dp_count * 8), 0))
        & (inner < per_device)
    )
    lax.fori_loop(1, dp_count, wait_row, 0)
    grouped = got_ref[...].astype(F32).reshape(dp_count * 8, 2 * LANES).astype(BF16)

    wait_exchange(*early_gate)
    gate_lines = gate_in[...].astype(F32).reshape(count * 8, LANES).astype(BF16)
    lines_upper, lines_lower = split_pair(mm(pick_lines, gate_lines))
    by_rank = mm(lines_upper, to_lane) + mm(lines_lower, to_lane)
    by_rank = jnp.sum(jnp.where(from_owner, by_rank, 0.0), axis=0, keepdims=True)
    picked = jnp.zeros((tokens, experts), F32)
    for r in range(depth):
        picked = picked + jnp.where(
            ranked == float(r + 1), by_rank[:, r * experts : (r + 1) * experts], 0.0
        )
    mixture = jnp.sum(picked * gates, axis=1, keepdims=True)
    d_chosen = hot * (route_scale * picked - mixture) / total
    logit_grad = (d_chosen * scores * (1.0 - scores)).astype(BF16)
    spread8 = mm(mm_nt(repeat8, logit_grad).astype(BF16), widen).astype(BF16)
    terms = mm(spread8, grouped)
    shift = lax.rem(mine * feature_share, LANES)
    terms = pltpu.roll(terms, lax.rem(2 * LANES - shift, 2 * LANES), 1)
    line8 = iota((count * 8, LANES), 0)
    line8 = line8 - over(line8, 8) * 8
    term_out[...] = jnp.where(
        line8 < local_experts, terms[:, :LANES], terms[:, LANES:]
    ).reshape(count, 8, LANES)
    start_exchange(*term)
    term_in[me] = term_out[me]

    wait_exchange(*back)
    mixed = mm(mix_ref[...], back_in[...].reshape(span, LANES))
    lane_of = over(iota((tokens, LANES), 1), TAIL)
    tails = jnp.zeros((tokens, LANES), F32)
    for e in range(local_experts):
        at_row = 2 * e * tokens
        both = mixed[at_row : at_row + tokens] + mixed[at_row + tokens : at_row + 2 * tokens]
        tails = tails + jnp.where(lane_of == e, both, 0.0)
    folded = tails
    for e in range(1, local_experts):
        folded = folded + pltpu.roll(tails, LANES - e * TAIL, 1)
    at_row = 2 * local_experts * tokens
    main = mixed[at_row : at_row + tokens] + mixed[at_row + tokens : at_row + 2 * tokens]
    main = main + mm_nt(logit_grad, router_weight_ref[:LANES, :])
    side = folded[:, :TAIL] + mm_nt(logit_grad, router_weight_ref[LANES:feature_share, :])
    grad_input_ref[:, :LANES] = main.astype(BF16)
    grad_input_ref[:, LANES:feature_share] = side.astype(BF16)

    for step in range(half):
        for g in range(parts):
            for way in range(2):
                if runs(way, half - step, g):
                    hop(way, step, g).wait_send()
                if runs(way, step + 1, g):
                    gather(way, step, g).wait_send()
    for g in range(parts):
        swap(g).wait_send()

    wait_exchange(*term)
    sums = jnp.sum(term_in[...], axis=0)
    grad_router_ref[:, :LANES] = sums[:local_experts]
    grad_router_ref[:, LANES:feature_share] = sums[local_experts : 2 * local_experts, :TAIL]


def hand_over(grad_input_in, grad_router_in, grad_input_out, grad_router_out):
    grad_input_out[0] = grad_input_in[...]
    grad_router_out[...] = grad_router_in[...]


def local(
    grad_output,
    router_logits,
    expert_ids,
    router_input,
    router_weight,
    gate_weight,
    up_weight,
    down_weight,
    gate_saved,
    up_saved,
):
    count = lax.axis_size("expert")
    ring, dp_1 = lax.axis_size("dp_0"), lax.axis_size("dp_1")
    dp_count = ring * dp_1
    tokens, feature_share = grad_output.shape[1:]
    experts = router_logits.shape[2]
    local_experts, slot_count, width = gate_saved.shape
    depth = slot_count // count
    expert_rows = slot_count
    row_total = local_experts * slot_count
    block_rows = row_total // ring
    parts = block_rows // 16
    half = ring // 2
    span = count * PIECE
    blocked = (ring, block_rows, width)
    hops = pltpu.SemaphoreType.DMA((2, half, parts))
    swaps = pltpu.SemaphoreType.DMA((parts,))
    peers = pltpu.SemaphoreType.DMA((count,))
    dp_peers = pltpu.SemaphoreType.DMA((dp_count,))
    grad_input, grad_router = pl.pallas_call(
        functools.partial(layer_kernel, (count, ring, dp_1, local_experts, depth, parts)),
        out_shape=(
            jax.ShapeDtypeStruct((tokens, feature_share), BF16),
            jax.ShapeDtypeStruct((local_experts, feature_share), F32),
        ),
        in_specs=[HBM] * 10,
        out_specs=(VMEM, VMEM),
        scratch_shapes=[
            pltpu.VMEM((tokens, feature_share), BF16),
            pltpu.VMEM(expert_ids.shape[:0:-1], jnp.int32),
            pltpu.VMEM((tokens, experts), F32),
            pltpu.VMEM(router_input.shape[1:], BF16),
            pltpu.VMEM(router_weight.shape[::-1], BF16),
            pltpu.VMEM((8, router_input.shape[2]), BF16),
            pltpu.VMEM((local_experts, 2 * LANES, width), BF16),
            pltpu.VMEM((local_experts, 2 * LANES, width), BF16),
            pltpu.VMEM((local_experts, 2 * LANES, width), BF16),
            pltpu.VMEM(blocked, BF16),
            pltpu.VMEM(blocked, BF16),
            pltpu.VMEM(blocked, F32),
            pltpu.VMEM(blocked, F32),
            pltpu.VMEM(blocked, BF16),
            pltpu.VMEM(blocked, F32),
            pltpu.VMEM(blocked, BF16),
            pltpu.VMEM((2, half, block_rows, width), BF16),
            pltpu.VMEM((2, half, block_rows, width), BF16),
            pltpu.VMEM((2, block_rows, width), BF16),
            pltpu.VMEM((count, PIECE, LANES), BF16),
            pltpu.VMEM((count, PIECE, LANES), BF16),
            pltpu.VMEM((row_total, LANES), BF16),
            pltpu.VMEM((expert_rows, LANES), BF16),
            pltpu.VMEM((block_rows, width), BF16),
            pltpu.VMEM((block_rows, width), BF16),
            pltpu.VMEM((row_total, LANES), BF16),
            pltpu.VMEM((expert_rows, LANES), F32),
            pltpu.VMEM((row_total, LANES), BF16),
            pltpu.VMEM((row_total, LANES), BF16),
            pltpu.VMEM((count, 8, LANES), BF16),
            pltpu.VMEM((count, 8, LANES), BF16),
            pltpu.VMEM((count, PIECE, LANES), BF16),
            pltpu.VMEM((count, PIECE, LANES), BF16),
            pltpu.VMEM(((local_experts + 1) * 2 * tokens, span), BF16),
            pltpu.VMEM((dp_count, 8, 2 * LANES), BF16),
            pltpu.VMEM((count, 8, LANES), F32),
            pltpu.VMEM((count, 8, LANES), F32),
            pltpu.SemaphoreType.DMA((5,)),
            pltpu.SemaphoreType.DMA((3 * 2 * local_experts + 2,)),
            hops,
            hops,
            swaps,
            swaps,
            hops,
            hops,
            peers,
            peers,
            peers,
            peers,
            peers,
            peers,
            peers,
            peers,
            dp_peers,
            dp_peers,
        ],
        compiler_params=pltpu.CompilerParams(
            collective_id=0, has_side_effects=True, vmem_limit_bytes=60 << 20
        ),
    )(
        grad_output[0],
        expert_ids[0].T,
        router_logits[0],
        router_input[0],
        router_weight.T,
        gate_weight,
        up_weight,
        jnp.swapaxes(down_weight, 1, 2),
        gate_saved.reshape(blocked),
        up_saved.reshape(blocked),
    )
    return pl.pallas_call(
        hand_over,
        out_shape=(
            jax.ShapeDtypeStruct((1, tokens, feature_share), BF16),
            jax.ShapeDtypeStruct((local_experts, feature_share), F32),
        ),
        in_specs=[VMEM, VMEM],
        out_specs=(VMEM, VMEM),
    )(grad_input, grad_router)


def solution(mesh):
    torus = Mesh(
        mesh.devices.reshape(mesh.shape["dp"] // 2, 2, mesh.shape["expert"]),
        ("dp_0", "dp_1", "expert"),
    )
    placed = (
        P("expert", None, DP),
        P("expert", None, None),
        P("expert", None, None),
        P("expert", DP, None),
        P(None, DP),
        P("expert", DP, None),
        P("expert", DP, None),
        P("expert", None, DP),
        P("expert", None, None),
        P("expert", None, None),
    )
    return jax.shard_map(
        local,
        mesh=torus,
        in_specs=placed,
        out_specs=(P("expert", None, DP), P("expert", DP)),
        check_vma=False,
    )
```

```python
import functools

import jax
import jax.numpy as jnp
from jax import lax
from jax.experimental import pallas as pl
from jax.experimental.pallas import tpu as pltpu
from jax.sharding import Mesh
from jax.sharding import PartitionSpec as P

DP = ("dp_0", "dp_1")
MESH = pl.DeviceIdType.MESH
VMEM = pl.BlockSpec(memory_space=pltpu.VMEM)
HBM = pl.BlockSpec(memory_space=pl.ANY)
F32, BF16 = jnp.float32, jnp.bfloat16
LANES = 128
TAIL = 32
PIECE = 32
CHUNK = 8

route_scale = 2.5


def iota(shape, dim):
    return lax.broadcasted_iota(jnp.int32, shape, dim)


def over(values, by):
    if by & (by - 1) == 0:
        return lax.shift_right_logical(values, jnp.full_like(values, by.bit_length() - 1))
    return lax.shift_right_logical(values * (65536 // by + 1), jnp.full_like(values, 16))


def hot_of(condition):
    return jnp.where(condition, 1.0, 0.0).astype(BF16)


def mm(a, b):
    return jnp.dot(a, b, preferred_element_type=F32)


def mm_nt(a, b):
    return lax.dot_general(a, b, (((1,), (1,)), ((), ())), preferred_element_type=F32)


def split_pair(values):
    upper = values.astype(BF16)
    return upper, (values - upper.astype(F32)).astype(BF16)


def layer_kernel(
    shape,
    rows_hbm,
    ids_hbm,
    logits_hbm,
    router_hbm,
    router_weight_hbm,
    gate_hbm,
    up_hbm,
    down_hbm,
    saved_gate_hbm,
    saved_up_hbm,
    grad_input_ref,
    grad_router_ref,
    rows_ref,
    ids_ref,
    logits_ref,
    router_in,
    router_weight_ref,
    router_ref,
    gate_w,
    up_w,
    down_w,
    saved_gate,
    saved_up,
    gate_factor,
    up_factor,
    hidden_ref,
    own_ref,
    sum_ref,
    send_buf,
    recv_buf,
    swap_buf,
    out_piece,
    in_piece,
    x_main,
    x_tail,
    part_gate,
    part_up,
    e_main,
    e_tail,
    g_upper,
    g_lower,
    gate_out,
    gate_in,
    back_out,
    back_in,
    mix_ref,
    got_ref,
    term_out,
    term_in,
    small_sem,
    load_sem,
    send_sem,
    recv_sem,
    swap_send,
    swap_recv,
    gsend,
    grecv,
    piece_send,
    piece_recv,
    gate_send,
    gate_recv,
    back_send,
    back_recv,
    term_send,
    term_recv,
    row_send,
    row_recv,
):
    count, ring, dp_1, local_experts, depth, parts = shape
    me, z, h = lax.axis_index("expert"), lax.axis_index("dp_0"), lax.axis_index("dp_1")
    dp_count = ring * dp_1
    mine = z * dp_1 + h
    tokens, experts = logits_hbm.shape
    feature_share = LANES + TAIL
    half = ring // 2
    block_rows, width = own_ref.shape[1:]
    expert_rows = count * depth
    rows = block_rows // parts
    per_expert = expert_rows // block_rows
    per_device = tokens // dp_count
    gate_row = local_experts * depth + depth
    neighbour = ({"dp_0": lax.rem(z + 1, ring)}, {"dp_0": lax.rem(z + ring - 1, ring)})
    partner = {"dp_1": 1 - h}

    def loads():
        copies = []
        for n, (hbm, to) in enumerate(((down_hbm, down_w), (gate_hbm, gate_w), (up_hbm, up_w))):
            for e in range(local_experts):
                for part, (at, size, put) in enumerate(
                    ((0, LANES, 0), (LANES, TAIL, LANES + e * TAIL))
                ):
                    copies.append(
                        pltpu.make_async_copy(
                            hbm.at[e, pl.ds(at, size)],
                            to.at[e, pl.ds(put, size)],
                            load_sem.at[n * 2 * local_experts + 2 * e + part],
                        )
                    )
        last = 3 * 2 * local_experts
        copies.append(pltpu.make_async_copy(saved_gate_hbm, saved_gate, load_sem.at[last]))
        copies.append(pltpu.make_async_copy(saved_up_hbm, saved_up, load_sem.at[last + 1]))
        return copies

    small = [
        pltpu.make_async_copy(hbm, to, small_sem.at[n])
        for n, (hbm, to) in enumerate(
            (
                (ids_hbm, ids_ref),
                (rows_hbm, rows_ref),
                (router_hbm, router_in),
                (logits_hbm, logits_ref),
                (router_weight_hbm, router_weight_ref),
            )
        )
    ]
    for copy in small:
        copy.start()

    barrier = pltpu.get_barrier_semaphore()

    def dp_peer(k):
        peer = lax.rem(mine + k, dp_count)
        return {"dp_0": peer // dp_1, "dp_1": lax.rem(peer, dp_1)}

    def greet_expert(k, carry):
        pl.semaphore_signal(
            barrier, inc=1, device_id={"expert": lax.rem(me + k, count)}, device_id_type=MESH
        )
        return carry

    def greet_dp(k, carry):
        pl.semaphore_signal(barrier, inc=1, device_id=dp_peer(k), device_id_type=MESH)
        return carry

    lax.fori_loop(1, dp_count, greet_dp, 0)
    lax.fori_loop(1, count, greet_expert, 0)
    load = loads()
    down_loads, late_loads, saved_loads = load[:8], load[8:24], load[24:]
    for copy in down_loads + saved_loads + late_loads:
        copy.start()

    small[0].wait()
    hot_t = jnp.zeros((experts, tokens), F32)
    for k in range(ids_ref.shape[0]):
        hot_t = hot_t + jnp.where(
            iota((experts, tokens), 0) == ids_ref[k : k + 1, :], 1.0, 0.0
        )
    earlier = hot_of(iota((tokens, tokens), 0) < iota((tokens, tokens), 1))
    ranked_t = (hot_t * (mm(hot_t.astype(BF16), earlier) + 1.0)).astype(BF16)

    main_rows = count * local_experts * depth
    row, col = iota((main_rows, experts), 0), iota((main_rows, experts), 1)
    values = mm(hot_of(over(row, depth) == col), ranked_t)
    wanted = iota((main_rows, tokens), 0)
    wanted = (wanted - over(wanted, depth) * depth + 1).astype(F32)
    small[1].wait()
    piece_main = mm(hot_of(values == wanted), rows_ref[:, :LANES])
    tail_rows = count * 8
    row, col = iota((tail_rows, experts), 0), iota((tail_rows, experts), 1)
    rank_of = iota((tail_rows, tokens), 0)
    rank_of = rank_of - over(rank_of, 8) * 8
    wanted = jnp.where(rank_of < depth, rank_of + 1, depth + 1000).astype(F32)
    piece_tail = jnp.zeros((tail_rows, LANES), F32)
    for e in range(local_experts):
        values = mm(hot_of(over(row, 8) * local_experts + e == col), ranked_t)
        lanes = hot_of(iota((TAIL, LANES), 0) + e * TAIL == iota((TAIL, LANES), 1))
        placed = mm(rows_ref[:, LANES:feature_share], lanes).astype(BF16)
        piece_tail = piece_tail + mm(hot_of(values == wanted), placed)
    out_piece[...] = jnp.concatenate(
        [
            piece_main.reshape(count, local_experts * depth, LANES),
            piece_tail.reshape(count, 8, LANES),
        ],
        axis=1,
    ).astype(BF16)

    small[2].wait()
    router_ref[...] = jnp.concatenate(
        [
            router_in[...].astype(F32),
            jnp.zeros((8 - per_device, router_in.shape[1]), F32),
        ],
        axis=0,
    ).astype(BF16)

    pl.semaphore_wait(barrier, count - 1 + dp_count - 1)

    def exchange(k, src, dst, send, recv):
        peer = lax.rem(me + k, count)
        return pltpu.make_async_remote_copy(
            src_ref=src.at[peer],
            dst_ref=dst.at[me],
            send_sem=send.at[k],
            recv_sem=recv.at[k],
            device_id={"expert": peer},
            device_id_type=MESH,
        )

    def start_exchange(*refs):
        def start(n, carry):
            away = (n + 1) // 2
            exchange(count // 2 + away * (2 * lax.rem(n, 2) - 1), *refs).start()
            return carry

        lax.fori_loop(0, count - 1, start, 0)

    def wait_exchange(*refs):
        def wait(k, carry):
            exchange(k, *refs).wait()
            return carry

        lax.fori_loop(1, count, wait, 0)

    piece = (out_piece, in_piece, piece_send, piece_recv)
    early_gate = (gate_out, gate_in, gate_send, gate_recv)
    back = (back_out, back_in, back_send, back_recv)
    term = (term_out, term_in, term_send, term_recv)
    start_exchange(*piece)
    in_piece[me] = out_piece[me]

    def window(peer):
        return pl.multiple_of(peer * feature_share // LANES * LANES, LANES)

    def row_copy(k):
        peer = lax.rem(mine + k, dp_count)
        return pltpu.make_async_remote_copy(
            src_ref=router_ref.at[:, pl.ds(window(peer), 2 * LANES)],
            dst_ref=got_ref.at[mine],
            send_sem=row_send.at[k],
            recv_sem=row_recv.at[k],
            device_id=dp_peer(k),
            device_id_type=MESH,
        )

    def start_row(k, carry):
        row_copy(k).start()
        return carry

    def wait_row(k, carry):
        row_copy(k).wait()
        return carry

    lax.fori_loop(1, dp_count, start_row, 0)
    got_ref[mine] = router_ref[:, pl.ds(window(mine), 2 * LANES)]

    for copy in small[3:]:
        copy.wait()
    for to in (down_w, gate_w, up_w):
        for e in range(local_experts):
            first = LANES + e * TAIL
            if e:
                to[e, LANES:first, :] = jnp.zeros((e * TAIL, width), BF16)
            if e < local_experts - 1:
                size = (local_experts - 1 - e) * TAIL
                to[e, first + TAIL : first + TAIL + size, :] = jnp.zeros((size, width), BF16)

    same = hot_of(iota((tokens, tokens), 0) == iota((tokens, tokens), 1))
    ranked = mm_nt(same, ranked_t)
    hot = jnp.where(ranked > 0.0, 1.0, 0.0)
    scores = 1.0 / (1.0 + jnp.exp(-logits_ref[...]))
    total = jnp.sum(scores * hot, axis=1, keepdims=True)
    gates = route_scale * (scores * hot) / total
    gate_upper, gate_lower = split_pair(gates)
    ranked_b = ranked.astype(BF16)
    span = count * PIECE
    slot = iota((experts, span), 1)
    inside = slot - over(slot, PIECE) * PIECE
    named = iota((experts, span), 0)
    line = iota((tokens, span), 1)
    line = line - over(line, PIECE) * PIECE
    line_rank = line - over(line, depth) * depth
    for e in range(local_experts + 1):
        if e == local_experts:
            of_expert = over(slot, PIECE) * local_experts + over(inside, depth)
            take = inside < local_experts * depth
            wanted = jnp.where(line < local_experts * depth, line_rank + 1, depth + 1000)
        else:
            of_expert = over(slot, PIECE) * local_experts + e
            take = (inside >= local_experts * depth) & (inside < gate_row)
            wanted = jnp.where(
                (line >= local_experts * depth) & (line < gate_row), line_rank + 1, depth + 1000
            )
        spread = hot_of((of_expert == named) & take)
        holds = mm(ranked_b, spread) == wanted.astype(F32)
        for n, part in enumerate((gate_upper, gate_lower)):
            at = (2 * e + n) * tokens
            mix_ref[at : at + tokens, :] = jnp.where(holds, mm(part, spread), 0.0).astype(BF16)

    for copy in saved_loads:
        copy.wait()

    def factors(block):
        def some(n, carry):
            at = pl.ds(pl.multiple_of(n * 16, 16), 16)
            gate_value = saved_gate[block, at, :].astype(F32)
            up_value = saved_up[block, at, :].astype(F32)
            sigmoid = 1.0 / (1.0 + jnp.exp(-gate_value))
            active = gate_value * sigmoid
            hidden_ref[block, at, :] = (active * up_value).astype(BF16)
            gate_factor[block, at, :] = (
                up_value * sigmoid * (1.0 + gate_value * (1.0 - sigmoid))
            )
            up_factor[block, at, :] = active
            return carry

        lax.fori_loop(0, block_rows // 16, some, 0)

    early = max(ring - half - 2, 0)
    for block in range(early):
        factors(block)

    chunk_rows = CHUNK * depth
    order_rows = (local_experts + 1) * chunk_rows

    def source(values):
        of_expert = over(values, chunk_rows)
        within = values - of_expert * chunk_rows
        group = over(within, depth)
        return group * PIECE + of_expert * depth + within - group * depth

    order_in = hot_of(
        source(iota((order_rows, CHUNK * PIECE), 0)) == iota((order_rows, CHUNK * PIECE), 1)
    )
    for copy in down_loads:
        copy.wait()
    wait_exchange(*piece)
    for n in range(count // CHUNK):
        chunk = in_piece[n * CHUNK : (n + 1) * CHUNK].reshape(CHUNK * PIECE, LANES)
        ordered = mm(order_in, chunk).astype(BF16)
        for e in range(local_experts):
            at = e * expert_rows + n * chunk_rows
            x_main[at : at + chunk_rows, :] = ordered[e * chunk_rows : (e + 1) * chunk_rows]
        x_tail[n * chunk_rows : (n + 1) * chunk_rows, :] = ordered[local_experts * chunk_rows :]

    def at(way, distance):
        step = distance if way == 0 else ring - distance
        return lax.rem(z + step, ring)

    def part(g):
        return pl.ds(g * rows, rows)

    def runs(way, distance, g):
        if distance < half:
            return True
        return (g < parts // 2) == (way == 0)

    def hop(way, step, g):
        return pltpu.make_async_remote_copy(
            src_ref=send_buf.at[way, step, part(g)],
            dst_ref=recv_buf.at[way, step, part(g)],
            send_sem=send_sem.at[way, step, g],
            recv_sem=recv_sem.at[way, step, g],
            device_id=neighbour[way],
            device_id_type=MESH,
        )

    def swap(g):
        return pltpu.make_async_remote_copy(
            src_ref=swap_buf.at[0, part(g)],
            dst_ref=swap_buf.at[1, part(g)],
            send_sem=swap_send.at[g],
            recv_sem=swap_recv.at[g],
            device_id=partner,
            device_id_type=MESH,
        )

    def gather(way, step, g):
        block = at(1 - way, step) if step else z
        return pltpu.make_async_remote_copy(
            src_ref=sum_ref.at[block, part(g)],
            dst_ref=sum_ref.at[block, part(g)],
            send_sem=gsend.at[way, step, g],
            recv_sem=grecv.at[way, step, g],
            device_id=neighbour[way],
            device_id_type=MESH,
        )

    far = lax.rem(z + half, ring)
    far_expert = far // per_expert
    far_tail = pl.ds(pl.multiple_of(lax.rem(far, per_expert) * block_rows, block_rows), block_rows)
    far_rows = pl.ds(pl.multiple_of(far * block_rows, block_rows), block_rows)
    first = jnp.concatenate([x_main[far_rows, :], x_tail[far_tail, :]], axis=1)
    first = mm(first, down_w[far_expert]).astype(BF16)
    for way in range(2):
        for g in range(parts):
            if runs(way, half, g):
                send_buf[way, 0, part(g), :] = first[g * rows : (g + 1) * rows]
                hop(way, 0, g).start()
    for e in range(local_experts):
        inputs = jnp.concatenate(
            [x_main[e * expert_rows : (e + 1) * expert_rows, :], x_tail[...]], axis=1
        )
        terms = mm(inputs, down_w[e])
        for n in range(per_expert):
            own_ref[e * per_expert + n] = terms[n * block_rows : (n + 1) * block_rows]

    for step in range(1, half):
        distance = half - step
        for g in range(parts):
            for way in range(2):
                value = own_ref[at(way, distance), part(g), :]
                if runs(way, distance + 1, g):
                    hop(way, step - 1, g).wait_recv()
                    value = value + recv_buf[way, step - 1, part(g), :].astype(F32)
                send_buf[way, step, part(g), :] = value.astype(BF16)
                hop(way, step, g).start()
        if early + step - 1 < ring:
            factors(early + step - 1)
    for g in range(parts):
        value = own_ref[z, part(g), :]
        for way in range(2):
            if runs(way, 1, g):
                hop(way, half - 1, g).wait_recv()
                value = value + recv_buf[way, half - 1, part(g), :].astype(F32)
        own_ref[z, part(g), :] = value
        swap_buf[0, part(g), :] = value.astype(BF16)
        swap(g).start()
    for block in range(early + half - 1, ring):
        factors(block)
    for copy in late_loads:
        copy.wait()
    e_tail[...] = jnp.zeros_like(e_tail)
    for g in range(parts):
        swap(g).wait_recv()
        total_sum = own_ref[z, part(g), :] + swap_buf[1, part(g), :].astype(F32)
        sum_ref[z, part(g), :] = total_sum.astype(BF16)
        for way in range(2):
            if runs(way, 1, g):
                gather(way, 0, g).start()

    def activate(block):
        of_expert = block // per_expert
        first_row = lax.rem(block, per_expert) * block_rows
        gate_rows = []
        for n in range(block_rows // 16):
            cut = slice(n * 16, (n + 1) * 16)
            value = sum_ref[block, cut, :].astype(F32)
            gate_rows.append(
                jnp.sum(hidden_ref[block, cut, :].astype(F32) * value, axis=1, keepdims=True)
            )
            part_gate[cut, :] = (value * gate_factor[block, cut, :]).astype(BF16)
            part_up[cut, :] = (value * up_factor[block, cut, :]).astype(BF16)
        gate_sum = jnp.concatenate(gate_rows, axis=0)
        block_at = pl.ds(pl.multiple_of(block * block_rows, block_rows), block_rows)
        place = iota((block_rows, LANES), 0) + first_row
        place = place - over(place, depth) * depth + of_expert * depth
        held = place == iota((block_rows, LANES), 1)
        upper, lower = split_pair(jnp.broadcast_to(gate_sum, (block_rows, LANES)))
        zero = jnp.zeros((block_rows, LANES), F32)
        g_upper[block_at, :] = jnp.where(held, upper.astype(F32), zero).astype(BF16)
        g_lower[block_at, :] = jnp.where(held, lower.astype(F32), zero).astype(BF16)

    def multiply(block):
        of_expert = block // per_expert
        first_row = lax.rem(block, per_expert) * block_rows
        out = mm_nt(part_gate[...], gate_w[of_expert]) + mm_nt(part_up[...], up_w[of_expert])
        block_at = pl.ds(pl.multiple_of(block * block_rows, block_rows), block_rows)
        tail_at = pl.ds(pl.multiple_of(first_row, block_rows), block_rows)
        e_main[block_at, :] = out[:, :LANES].astype(BF16)
        e_tail[tail_at, :] = e_tail[tail_at, :] + out[:, LANES:]

    def project(block):
        activate(block)
        multiply(block)

    waiting = [z]
    for step in range(1, half):
        for g in range(parts):
            for way in range(2):
                gather(way, step - 1, g).wait_recv()
                if runs(way, step + 1, g):
                    gather(way, step, g).start()
            if g in (parts // 2 - 1, parts - 1) and waiting:
                project(waiting.pop(0))
        waiting += [at(1, step), at(0, step)]
    for block in waiting:
        project(block)

    chunk_lines = CHUNK * 8
    gate_cols = local_experts * chunk_rows
    group_of = iota((chunk_lines, gate_cols), 1)
    group_of = over(group_of - over(group_of, chunk_rows) * chunk_rows, depth) * 8
    line_of = iota((chunk_lines, gate_cols), 0)
    order_upper = hot_of(group_of == line_of)
    order_lower = hot_of(group_of + 1 == line_of)
    piece_of = iota((CHUNK * PIECE, order_rows), 0)
    order_out = hot_of(source(iota((CHUNK * PIECE, order_rows), 1)) == piece_of)

    def cut_of(ref, n):
        return [
            ref[e * expert_rows + n * chunk_rows : e * expert_rows + (n + 1) * chunk_rows, :]
            for e in range(local_experts)
        ]

    for g in range(parts):
        for way in range(2):
            if runs(way, half, g):
                gather(way, half - 1, g).wait_recv()
    activate(far)
    for n in range(count // CHUNK):
        lines = mm(order_upper, jnp.concatenate(cut_of(g_upper, n), axis=0))
        lines = lines + mm(order_lower, jnp.concatenate(cut_of(g_lower, n), axis=0))
        gate_out[n * CHUNK : (n + 1) * CHUNK] = lines.reshape(CHUNK, 8, LANES).astype(BF16)
    start_exchange(*early_gate)
    gate_in[me] = gate_out[me]
    multiply(far)
    for n in range(count // CHUNK):
        tail = e_tail[n * chunk_rows : (n + 1) * chunk_rows, :].astype(BF16)
        pieces = mm(order_out, jnp.concatenate([*cut_of(e_main, n), tail], axis=0))
        back_out[n * CHUNK : (n + 1) * CHUNK] = pieces.astype(BF16).reshape(CHUNK, PIECE, LANES)
    start_exchange(*back)
    back_in[me] = back_out[me]

    gate_lines = iota((count, count * 8), 1) - iota((count, count * 8), 0) * 8
    pick_lines = hot_of((gate_lines == 0) | (gate_lines == 1))
    lane, to = iota((LANES, depth * experts), 0), iota((LANES, depth * experts), 1)
    to_rank = over(to, experts)
    to_expert = to - to_rank * experts
    to_local = to_expert - over(to_expert, local_experts) * local_experts
    to_lane = hot_of(lane == to_local * depth + to_rank)
    to = iota((count, depth * experts), 1)
    to_expert = to - over(to, experts) * experts
    from_owner = over(to_expert, local_experts) == iota((count, depth * experts), 0)
    line8 = iota((count * 8, experts), 0)
    owner8 = over(line8, 8)
    inner8 = line8 - owner8 * 8
    inner8 = inner8 - over(inner8, local_experts) * local_experts
    repeat8 = hot_of(owner8 * local_experts + inner8 == iota((count * 8, experts), 1))
    token8 = iota((tokens, dp_count * 8), 1)
    inner = token8 - over(token8, 8) * 8
    widen = hot_of(
        (over(token8, 8) * per_device + inner == iota((tokens, dp_count * 8), 0))
        & (inner < per_device)
    )
    lax.fori_loop(1, dp_count, wait_row, 0)
    grouped = got_ref[...].astype(F32).reshape(dp_count * 8, 2 * LANES).astype(BF16)

    wait_exchange(*early_gate)
    gate_lines = gate_in[...].astype(F32).reshape(count * 8, LANES).astype(BF16)
    lines_upper, lines_lower = split_pair(mm(pick_lines, gate_lines))
    by_rank = mm(lines_upper, to_lane) + mm(lines_lower, to_lane)
    by_rank = jnp.sum(jnp.where(from_owner, by_rank, 0.0), axis=0, keepdims=True)
    picked = jnp.zeros((tokens, experts), F32)
    for r in range(depth):
        picked = picked + jnp.where(
            ranked == float(r + 1), by_rank[:, r * experts : (r + 1) * experts], 0.0
        )
    mixture = jnp.sum(picked * gates, axis=1, keepdims=True)
    d_chosen = hot * (route_scale * picked - mixture) / total
    logit_grad = (d_chosen * scores * (1.0 - scores)).astype(BF16)
    spread8 = mm(mm_nt(repeat8, logit_grad).astype(BF16), widen).astype(BF16)
    terms = mm(spread8, grouped)
    shift = lax.rem(mine * feature_share, LANES)
    terms = pltpu.roll(terms, lax.rem(2 * LANES - shift, 2 * LANES), 1)
    line8 = iota((count * 8, LANES), 0)
    line8 = line8 - over(line8, 8) * 8
    term_out[...] = jnp.where(
        line8 < local_experts, terms[:, :LANES], terms[:, LANES:]
    ).reshape(count, 8, LANES)
    start_exchange(*term)
    term_in[me] = term_out[me]

    wait_exchange(*back)
    mixed = mm(mix_ref[...], back_in[...].reshape(span, LANES))
    lane_of = over(iota((tokens, LANES), 1), TAIL)
    tails = jnp.zeros((tokens, LANES), F32)
    for e in range(local_experts):
        at_row = 2 * e * tokens
        both = mixed[at_row : at_row + tokens] + mixed[at_row + tokens : at_row + 2 * tokens]
        tails = tails + jnp.where(lane_of == e, both, 0.0)
    folded = tails
    for e in range(1, local_experts):
        folded = folded + pltpu.roll(tails, LANES - e * TAIL, 1)
    at_row = 2 * local_experts * tokens
    main = mixed[at_row : at_row + tokens] + mixed[at_row + tokens : at_row + 2 * tokens]
    main = main + mm_nt(logit_grad, router_weight_ref[:LANES, :])
    side = folded[:, :TAIL] + mm_nt(logit_grad, router_weight_ref[LANES:feature_share, :])
    grad_input_ref[:, :LANES] = main.astype(BF16)
    grad_input_ref[:, LANES:feature_share] = side.astype(BF16)

    for step in range(half):
        for g in range(parts):
            for way in range(2):
                if runs(way, half - step, g):
                    hop(way, step, g).wait_send()
                if runs(way, step + 1, g):
                    gather(way, step, g).wait_send()
    for g in range(parts):
        swap(g).wait_send()

    wait_exchange(*term)
    sums = jnp.sum(term_in[...], axis=0)
    grad_router_ref[:, :LANES] = sums[:local_experts]
    grad_router_ref[:, LANES:feature_share] = sums[local_experts : 2 * local_experts, :TAIL]


def hand_over(grad_input_in, grad_router_in, grad_input_out, grad_router_out):
    grad_input_out[0] = grad_input_in[...]
    grad_router_out[...] = grad_router_in[...]


def local(
    grad_output,
    router_logits,
    expert_ids,
    router_input,
    router_weight,
    gate_weight,
    up_weight,
    down_weight,
    gate_saved,
    up_saved,
):
    count = lax.axis_size("expert")
    ring, dp_1 = lax.axis_size("dp_0"), lax.axis_size("dp_1")
    dp_count = ring * dp_1
    tokens, feature_share = grad_output.shape[1:]
    experts = router_logits.shape[2]
    local_experts, slot_count, width = gate_saved.shape
    depth = slot_count // count
    expert_rows = slot_count
    row_total = local_experts * slot_count
    block_rows = row_total // ring
    parts = block_rows // 16
    half = ring // 2
    span = count * PIECE
    blocked = (ring, block_rows, width)
    hops = pltpu.SemaphoreType.DMA((2, half, parts))
    swaps = pltpu.SemaphoreType.DMA((parts,))
    peers = pltpu.SemaphoreType.DMA((count,))
    dp_peers = pltpu.SemaphoreType.DMA((dp_count,))
    grad_input, grad_router = pl.pallas_call(
        functools.partial(layer_kernel, (count, ring, dp_1, local_experts, depth, parts)),
        out_shape=(
            jax.ShapeDtypeStruct((tokens, feature_share), BF16),
            jax.ShapeDtypeStruct((local_experts, feature_share), F32),
        ),
        in_specs=[HBM] * 10,
        out_specs=(VMEM, VMEM),
        scratch_shapes=[
            pltpu.VMEM((tokens, feature_share), BF16),
            pltpu.VMEM(expert_ids.shape[:0:-1], jnp.int32),
            pltpu.VMEM((tokens, experts), F32),
            pltpu.VMEM(router_input.shape[1:], BF16),
            pltpu.VMEM(router_weight.shape[::-1], BF16),
            pltpu.VMEM((8, router_input.shape[2]), BF16),
            pltpu.VMEM((local_experts, 2 * LANES, width), BF16),
            pltpu.VMEM((local_experts, 2 * LANES, width), BF16),
            pltpu.VMEM((local_experts, 2 * LANES, width), BF16),
            pltpu.VMEM(blocked, BF16),
            pltpu.VMEM(blocked, BF16),
            pltpu.VMEM(blocked, F32),
            pltpu.VMEM(blocked, F32),
            pltpu.VMEM(blocked, BF16),
            pltpu.VMEM(blocked, F32),
            pltpu.VMEM(blocked, BF16),
            pltpu.VMEM((2, half, block_rows, width), BF16),
            pltpu.VMEM((2, half, block_rows, width), BF16),
            pltpu.VMEM((2, block_rows, width), BF16),
            pltpu.VMEM((count, PIECE, LANES), BF16),
            pltpu.VMEM((count, PIECE, LANES), BF16),
            pltpu.VMEM((row_total, LANES), BF16),
            pltpu.VMEM((expert_rows, LANES), BF16),
            pltpu.VMEM((block_rows, width), BF16),
            pltpu.VMEM((block_rows, width), BF16),
            pltpu.VMEM((row_total, LANES), BF16),
            pltpu.VMEM((expert_rows, LANES), F32),
            pltpu.VMEM((row_total, LANES), BF16),
            pltpu.VMEM((row_total, LANES), BF16),
            pltpu.VMEM((count, 8, LANES), BF16),
            pltpu.VMEM((count, 8, LANES), BF16),
            pltpu.VMEM((count, PIECE, LANES), BF16),
            pltpu.VMEM((count, PIECE, LANES), BF16),
            pltpu.VMEM(((local_experts + 1) * 2 * tokens, span), BF16),
            pltpu.VMEM((dp_count, 8, 2 * LANES), BF16),
            pltpu.VMEM((count, 8, LANES), F32),
            pltpu.VMEM((count, 8, LANES), F32),
            pltpu.SemaphoreType.DMA((5,)),
            pltpu.SemaphoreType.DMA((3 * 2 * local_experts + 2,)),
            hops,
            hops,
            swaps,
            swaps,
            hops,
            hops,
            peers,
            peers,
            peers,
            peers,
            peers,
            peers,
            peers,
            peers,
            dp_peers,
            dp_peers,
        ],
        compiler_params=pltpu.CompilerParams(
            collective_id=0, has_side_effects=True, vmem_limit_bytes=60 << 20
        ),
    )(
        grad_output[0],
        expert_ids[0].T,
        router_logits[0],
        router_input[0],
        router_weight.T,
        gate_weight,
        up_weight,
        jnp.swapaxes(down_weight, 1, 2),
        gate_saved.reshape(blocked),
        up_saved.reshape(blocked),
    )
    return pl.pallas_call(
        hand_over,
        out_shape=(
            jax.ShapeDtypeStruct((1, tokens, feature_share), BF16),
            jax.ShapeDtypeStruct((local_experts, feature_share), F32),
        ),
        in_specs=[VMEM, VMEM],
        out_specs=(VMEM, VMEM),
    )(grad_input, grad_router)


def solution(mesh):
    torus = Mesh(
        mesh.devices.reshape(mesh.shape["dp"] // 2, 2, mesh.shape["expert"]),
        ("dp_0", "dp_1", "expert"),
    )
    placed = (
        P("expert", None, DP),
        P("expert", None, None),
        P("expert", None, None),
        P("expert", DP, None),
        P(None, DP),
        P("expert", DP, None),
        P("expert", DP, None),
        P("expert", None, DP),
        P("expert", None, None),
        P("expert", None, None),
    )
    return jax.shard_map(
        local,
        mesh=torus,
        in_specs=placed,
        out_specs=(P("expert", None, DP), P("expert", DP)),
        check_vma=False,
    )
```
